512 devices in a mesh: coil: 32 (over x, z), frame: 16 (over y, core).
Axes of the slice: x: 4, y: 8, z: 8, core: 2. Of those that a mesh axis runs over, the one named last changes fastest.
Arguments:
- initial_image: float32 [256, 16, 2, 256], P('coil', 'frame'), may hold values from -3 to 3
- coil_maps: bfloat16 [32, 2, 256, 256], P('coil'), may hold values from -1.5 to 1.5
- samples: bfloat16 [32, 16, 18, 2, 256], P('coil', 'frame'), may hold values from -6 to 6
- blocks_used: int32 [16], P('frame'), may hold values from 1 to 18, 145 in all
- row_offset: int32 [16, 18], P('frame'), may hold values from 0 to 128
- col_offset: int32 [16, 18], P('frame'), may hold values from 0 to 128
- row_first: int32 [16, 18, 256], P('frame'), may hold values from 0 to 124
- col_first: int32 [16, 18, 256], P('frame'), may hold values from 0 to 124
- row_taps: bfloat16 [16, 18, 4, 256], P('frame'), may hold values from 0.099609375 to 0.59765625
- col_taps: bfloat16 [16, 18, 4, 256], P('frame'), may hold values from 0.099609375 to 0.59765625
Outputs:
- image: float32 [256, 16, 2, 256], P('coil', 'frame')
- misfit: float32 [2, 16], P(None, 'frame')
The draws below stay inside these ranges and needn't reach their ends.
Inputs may be any that keep to these rules, and one draw needn't show every extreme that they name: Blocks 0 to blocks_used minus one of the frame were acquired. `row_first`: the kernel's 4 rows lie inside the tile. `col_first`: the kernel's 4 columns lie inside the tile.
All inputs are finite; a program needn't handle non-finite values.
Results may differ from the reference program's by a relative error of at most 0.006.
Values may be sent and summed in bfloat16 or wider, within the bound.
A program may use at most 64 MiB of HBM per device.

```python
import math
import jax
import jax.numpy as jnp
import numpy as np
from jax import lax

N = 256
COILS = 32
FRAMES = 16
NB = 18
BS = 256
TT = 128
KW = 4
ITERS = 2


def touch_ends(drawn, own_key, least, largest):
    longest = drawn.shape.index(max(drawn.shape))
    spots = []
    for shift in (0, 1):
        where = [jax.random.randint(jax.random.fold_in(own_key, axis), (), 0, length) for axis, length in enumerate(drawn.shape)]
        where[longest] = (where[longest] + shift) % drawn.shape[longest]
        spots.append(tuple(where))
    return drawn.at[spots[0]].set(least).at[spots[1]].set(largest)


def spiked(array, rng, source, target, parts, factor):
    def block_of(axis_at):
        return (jnp.arange(array.shape[axis_at]) // (array.shape[axis_at] // parts)).reshape((-1,) + (1,) * (array.ndim - 1 - axis_at))

    first = jax.random.permutation(rng, parts)[block_of(target)]
    far = (block_of(target) + parts // 2) % parts
    return jnp.where((block_of(source) == first) | (block_of(source) == far), factor * array, array)


def level_of(stream_key, shape, cuts, low, top_value):
    def one(position, blocks):
        draws = jax.random.uniform(jax.random.fold_in(jax.random.fold_in(stream_key, 6), position), (blocks,), jnp.float32, low / len(cuts), top_value / len(cuts))
        return jnp.repeat(jnp.exp(draws), shape[position] // blocks).reshape((-1,) + (1,) * (len(shape) - position - 1))

    factor_of = one(*cuts[0])
    for cut in cuts[1:]:
        factor_of = factor_of * one(*cut)
    return factor_of


def length_profile(count, total, most, slope):
    portions = [(1 << 20) // math.isqrt(standing ** slope) + 1 for standing in range(2, count + 1)]
    rest, counts = total - most - (count - 1), [1] * (count - 1)
    while rest > 0:
        candidates = [i for i in range(count - 1) if counts[i] < most]
        mass, remaining = sum([portions[i] for i in candidates]), rest
        for i in candidates:
            addition = min(most - counts[i], max(1, remaining * portions[i] // mass), rest)
            counts[i] = counts[i] + addition
            rest = rest - addition
    return np.array([most] + counts)


def uneven_parts(stream_key, count, total, reach, lean):
    if count == 2:
        one = jax.random.randint(stream_key, (), max(1, total - reach), min(reach, total - 1) + 1)
        return jnp.stack([one, total - one])
    lengths = jnp.asarray(length_profile(count, total, reach, lean), jnp.int32)
    twos = (count - 1) // 2
    giver, sink = lengths[1:1 + 2 * twos:2], lengths[2:2 + 2 * twos:2]
    slack = jnp.minimum(giver - 1, reach - sink)
    passed = jax.random.randint(jax.random.fold_in(stream_key, 1), (twos,), 0, 1 << 20) % (slack + 1)
    lengths = lengths.at[1:1 + 2 * twos:2].set(giver - passed).at[2:2 + 2 * twos:2].set(sink + passed)
    return lengths[jax.random.permutation(jax.random.fold_in(stream_key, 2), count)]


def centred(rng, shape, width, most, shards=(), kind=jnp.bfloat16):
    gain = level_of(rng, shape, shards, -0.22, 0.18) if shards else 1.0
    drawn = jax.random.normal(rng, shape, jnp.float32) * width * gain
    return jnp.minimum(jnp.maximum(drawn, -most), most).astype(kind)


def bell_draw_with(stream_key, shape, deviation, most, shards, heavy, kind=jnp.bfloat16):
    entries = deviation * jax.random.normal(stream_key, shape, jnp.float32)
    if shards:
        entries = entries * level_of(stream_key, shape, shards, -0.22, 0.18)
    return jnp.clip(spiked(entries, jax.random.fold_in(stream_key, 3), *heavy), -most, most).astype(kind)


def setup_inputs(seed: int = 0) -> dict:
    key_list = jax.random.split(jax.random.key(seed), 11)
    return {
        "initial_image": centred(key_list[0], (N, FRAMES, 2, N), 0.5, 3.0, ((0, 32), (1, 16)), jnp.float32),
        "coil_maps": bell_draw_with(key_list[1], (COILS, 2, N, N), (2 * COILS) ** -0.5, 1.5, ((0, 32),), (0, 2, 32, 2.75)),
        "samples": centred(key_list[2], (COILS, FRAMES, NB, 2, BS), 1.0, 6.0, ((0, 32), (1, 16))),
        "blocks_used": uneven_parts(key_list[3], FRAMES, FRAMES * NB // 2 + 1, NB, 2).astype(jnp.int32),
        "row_offset": touch_ends(jax.random.randint(key_list[4], (FRAMES, NB), 0, N - TT + 1), jax.random.fold_in(key_list[4], 1), 0, N - TT).astype(jnp.int32),
        "col_offset": touch_ends(jax.random.randint(key_list[5], (FRAMES, NB), 0, N - TT + 1), jax.random.fold_in(key_list[5], 1), 0, N - TT).astype(jnp.int32),
        "row_first": touch_ends(jax.random.randint(key_list[6], (FRAMES, NB, BS), 0, TT - KW + 1), jax.random.fold_in(key_list[6], 1), 0, TT - KW).astype(jnp.int32),
        "col_first": touch_ends(jax.random.randint(key_list[7], (FRAMES, NB, BS), 0, TT - KW + 1), jax.random.fold_in(key_list[7], 1), 0, TT - KW).astype(jnp.int32),
        "row_taps": jnp.clip(0.099609375 + 0.49804688 * jax.random.uniform(key_list[8], (FRAMES, NB, KW, BS), jnp.float32) ** level_of(key_list[8], (FRAMES, NB, KW, BS), ((0, 16),), -0.2, 0.2), 0.099609375, 0.59765625).astype(jnp.bfloat16),
        "col_taps": jnp.clip(0.099609375 + 0.49804688 * jax.random.uniform(key_list[9], (FRAMES, NB, KW, BS), jnp.float32) ** level_of(key_list[9], (FRAMES, NB, KW, BS), ((0, 16),), -0.2, 0.2), 0.099609375, 0.59765625).astype(jnp.bfloat16),
    }


step_size = 2.0
tv_weight = 0.1
smooth_floor = 0.5
shrink_weight = 0.1

def rounded(values):
    return lax.optimization_barrier(values.astype(jnp.bfloat16))

def pair_tables(order):
    counter = jnp.arange(order, dtype=jnp.int32)
    phase = counter[:, None] * counter[None, :] % order
    angle = phase.astype(jnp.float32) * (2.0 * math.pi / order)
    cosine = (jnp.cos(angle) / math.sqrt(order)).astype(jnp.bfloat16)
    sine = (jnp.sin(angle) / math.sqrt(order)).astype(jnp.bfloat16)
    table_one = jnp.stack([jnp.stack([cosine, sine]), jnp.stack([-sine, cosine])])
    table_two = jnp.stack([jnp.stack([cosine, -sine]), jnp.stack([sine, cosine])])
    return (table_one, table_two)

def tap_matrix(first_idx, taps):
    positions = jnp.arange(TT, dtype=jnp.int32)
    matrix = jnp.zeros((first_idx.shape[0], TT), jnp.float32)
    for offset in range(KW):
        hits = positions[None, :] == first_idx[:, None] + offset
        matrix = matrix + jnp.where(hits, taps[offset].astype(jnp.float32)[:, None], 0.0)
    return matrix.astype(jnp.bfloat16)

def spoke_block(kspace, grid_sum, tile_row, tile_col, first_row, first_col, taps_row, taps_col, measured, active):
    rows_matrix = tap_matrix(first_row, taps_row)
    cols_matrix = tap_matrix(first_col, taps_col)
    anchor = jnp.zeros((), jnp.int32)
    corner = (anchor, tile_row.astype(jnp.int32), tile_col.astype(jnp.int32))
    grid_tile = lax.dynamic_slice(kspace, corner, (2, TT, TT))
    across = jnp.einsum('si,pij->psj', rows_matrix.astype(jnp.float32), grid_tile.astype(jnp.float32))
    cols_wide = cols_matrix.astype(jnp.float32)
    predicted = lax.optimization_barrier(jnp.sum(across * cols_wide[None], axis=2))
    resid = (predicted - measured.astype(jnp.float32)) * active
    misfit = jnp.sum(resid * resid)
    resid_low = rounded(resid)
    weighted = rounded(resid_low.astype(jnp.float32)[:, :, None] * cols_wide[None])
    spread = jnp.einsum('si,psj->pij', rows_matrix.astype(jnp.float32), weighted.astype(jnp.float32))
    updated = lax.dynamic_slice(grid_sum, corner, (2, TT, TT)) + spread
    return (lax.dynamic_update_slice(grid_sum, updated, corner), misfit)

def frame_grid(kspace, count, row_off, col_off, row_idx, col_idx, row_w, col_w, measured):

    def visit(running, inputs):
        grid_sum, misfit_sum = running
        block_id, tile_row, tile_col, first_row, first_col, taps_row, taps_col, block_data = inputs
        active = (block_id < count).astype(jnp.float32)
        grid_sum, misfit = spoke_block(kspace, grid_sum, tile_row, tile_col, first_row, first_col, taps_row, taps_col, block_data, active)
        return ((grid_sum, misfit_sum + misfit), None)
    initial = (jnp.zeros((2, N, N), jnp.float32), jnp.zeros((), jnp.float32))
    blocks = jnp.arange(NB, dtype=jnp.int32)
    (grid_sum, misfit_sum), unused = lax.scan(visit, initial, (blocks, row_off, col_off, row_idx, col_idx, row_w, col_w, measured))
    return (rounded(grid_sum), misfit_sum)

def coil_forward(image_low, maps, table_one, table_two):
    maps_wide = maps.astype(jnp.float32)
    image_wide = image_low.astype(jnp.float32)
    real_part = maps_wide[0][:, None, :] * image_wide[:, :, 0] - maps_wide[1][:, None, :] * image_wide[:, :, 1]
    imag_part = maps_wide[0][:, None, :] * image_wide[:, :, 1] + maps_wide[1][:, None, :] * image_wide[:, :, 0]
    coil_image = rounded(jnp.stack([real_part, imag_part], axis=2))
    half = rounded(jnp.einsum('qprk,kfpn->fqrn', table_one.astype(jnp.float32), coil_image.astype(jnp.float32)))
    return rounded(jnp.einsum('fprk,pqkn->fqrn', half.astype(jnp.float32), table_two.astype(jnp.float32)))

def coil_adjoint(grid_low, maps, table_one, table_two):
    back_half = rounded(jnp.einsum('qprk,fpkn->fqrn', table_two.astype(jnp.float32), grid_low.astype(jnp.float32)))
    coil_back = jnp.einsum('fprk,pqkn->rfqn', back_half.astype(jnp.float32), table_one.astype(jnp.float32))
    maps_wide = maps.astype(jnp.float32)
    real_part = maps_wide[0][:, None, :] * coil_back[:, :, 0] + maps_wide[1][:, None, :] * coil_back[:, :, 1]
    imag_part = maps_wide[0][:, None, :] * coil_back[:, :, 1] - maps_wide[1][:, None, :] * coil_back[:, :, 0]
    return jnp.stack([real_part, imag_part], axis=2)

def cine_gradient(padded):
    change = padded[:, 1:] - padded[:, :-1]
    length = jnp.sqrt(lax.optimization_barrier(jnp.sum(change * change, axis=2, keepdims=True)) + smooth_floor * smooth_floor)
    normed = change / length
    return normed[:, :-1] - normed[:, 1:]

def shrink(detail, limit):
    length = jnp.sqrt(lax.optimization_barrier(jnp.sum(detail * detail, axis=2, keepdims=True)))
    return detail * (jnp.maximum(length - limit, 0.0) / jnp.maximum(length, limit))

def wavelet_prox(field, limit):
    even_rows = field[0::2]
    odd_rows = field[1::2]
    top_left = even_rows[..., 0::2]
    top_right = even_rows[..., 1::2]
    low_left = odd_rows[..., 0::2]
    low_right = odd_rows[..., 1::2]
    approx = (top_left + top_right + low_left + low_right) * 0.5
    horiz = shrink((top_left - top_right + low_left - low_right) * 0.5, limit)
    vertical = shrink((top_left + top_right - low_left - low_right) * 0.5, limit)
    diagonal = shrink((top_left - top_right - low_left + low_right) * 0.5, limit)
    new_tl = (approx + horiz + vertical + diagonal) * 0.5
    new_tr = (approx - horiz + vertical - diagonal) * 0.5
    new_ll = (approx + horiz - vertical - diagonal) * 0.5
    new_lr = (approx - horiz - vertical + diagonal) * 0.5
    top_rows = jnp.stack([new_tl, new_tr], axis=-1).reshape(even_rows.shape)
    low_rows = jnp.stack([new_ll, new_lr], axis=-1).reshape(odd_rows.shape)
    return jnp.stack([top_rows, low_rows], axis=1).reshape(field.shape)

def reference(initial_image, coil_maps, samples, blocks_used, row_offset, col_offset, row_first, col_first, row_taps, col_taps):
    table_one, table_two = pair_tables(N)
    grid_frames = jax.vmap(frame_grid)

    def data_term(image_low):

        def per_coil(running, inputs):
            grad_sum, misfit_sum = running
            maps, measured = inputs
            kspace = coil_forward(image_low, maps, table_one, table_two)
            grid_low, misfit = grid_frames(kspace, blocks_used, row_offset, col_offset, row_first, col_first, row_taps, col_taps, measured)
            partial_image = coil_adjoint(grid_low, maps, table_one, table_two)
            return ((grad_sum + partial_image, misfit_sum + misfit), None)
        initial = (jnp.zeros(initial_image.shape, jnp.float32), jnp.zeros((FRAMES,), jnp.float32))
        totals, unused = lax.scan(per_coil, initial, (coil_maps, samples))
        return totals
    misfit_scale = 0.5 / (COILS * NB * BS)
    current = initial_image.astype(jnp.float32)
    moving = current
    momentum = 1.0
    misfit_rows = []
    for step_num in range(ITERS):
        data_grad, misfit = data_term(rounded(moving))
        misfit_rows.append(misfit * misfit_scale)
        padded = jnp.concatenate([moving[:, -1:], moving, moving[:, :1]], axis=1)
        descent = moving - step_size * (data_grad + tv_weight * cine_gradient(padded))
        updated = wavelet_prox(descent, step_size * shrink_weight)
        following = (1.0 + math.sqrt(1.0 + 4.0 * momentum * momentum)) / 2.0
        moving = updated + (momentum - 1.0) / following * (updated - current)
        current = updated
        momentum = following
    return (current, jnp.stack(misfit_rows))
```

```python
import functools
import math

import jax
import jax.numpy as jnp
import numpy as np
from jax import lax
from jax.experimental import pallas as pl
from jax.experimental.pallas import tpu as pltpu
from jax.sharding import PartitionSpec as P

N = 256
NB = 18
BS = 256
KW = 4
ITERS = 2

step_size = 2.0
tv_weight = 0.1
smooth_floor = 0.5
shrink_weight = 0.1

MESH = pl.DeviceIdType.MESH
F32 = jnp.float32
BF16 = jnp.bfloat16


def dft_tables():
    counter = np.arange(N)
    angle = (counter[:, None] * counter[None, :] % N) * (2.0 * math.pi / N)
    cosine = jnp.asarray((np.cos(angle) / math.sqrt(N)).astype(np.float32)).astype(BF16)
    sine = jnp.asarray((np.sin(angle) / math.sqrt(N)).astype(np.float32)).astype(BF16)
    return np.stack([np.asarray(cosine), np.asarray(sine), np.asarray(-sine)])


def mm(a, b):
    return jnp.dot(a, b, preferred_element_type=F32)


def mm_nt(a, b):
    return lax.dot_general(a, b, (((1,), (1,)), ((), ())), preferred_element_type=F32)


def taps_of(first, offset, taps):
    distance = lax.broadcasted_iota(jnp.int32, (N, BS), 0) - (first + offset)
    matrix = jnp.zeros((N, BS), F32)
    for tap in range(KW):
        matrix = jnp.where(distance == tap, taps[tap : tap + 1, :], matrix)
    return matrix.astype(BF16)


def swap_lanes(field):
    lane = lax.broadcasted_iota(jnp.int32, field.shape, 1)
    width = field.shape[1]
    return jnp.where(
        lane % 2 == 0, pltpu.roll(field, width - 1, 1), pltpu.roll(field, 1, 1)
    )


def swap_rows(field):
    row = lax.broadcasted_iota(jnp.int32, field.shape, 0)
    height = field.shape[0]
    return jnp.where(
        row % 2 == 0, pltpu.roll(field, height - 1, 0), pltpu.roll(field, 1, 0)
    )


def shrunk(real, imag, limit):
    length = jnp.sqrt(real * real + imag * imag)
    factor = jnp.maximum(length - limit, 0.0) / jnp.maximum(length, limit)
    return real * factor, imag * factor


def wavelet_prox(real, imag, limit):
    parts = []
    for field in (real, imag):
        across = swap_lanes(field)
        down = swap_rows(field)
        both = swap_lanes(down)
        parts.append(
            (
                (field + across + down + both) * 0.5,
                (field - across + down - both) * 0.5,
                (field + across - down - both) * 0.5,
                (field - across - down + both) * 0.5,
            )
        )
    out_real, out_imag = parts[0][0], parts[1][0]
    for band in range(1, 4):
        band_real, band_imag = shrunk(parts[0][band], parts[1][band], limit)
        out_real = out_real + band_real
        out_imag = out_imag + band_imag
    return out_real * 0.5, out_imag * 0.5


def slope(late, early):
    real = late[0] - early[0]
    imag = late[1] - early[1]
    length = jnp.sqrt(real * real + imag * imag + smooth_floor * smooth_floor)
    return real / length, imag / length


def kernel(
    coils,
    frames,
    image_ref,
    maps_ref,
    samples_ref,
    used_ref,
    row_off_ref,
    col_off_ref,
    row_first_ref,
    col_first_ref,
    row_taps_ref,
    col_taps_ref,
    table_ref,
    out_ref,
    misfit_ref,
    current,
    low,
    gathered,
    beside,
    part_out,
    part_in,
    mis_out,
    mis_in,
    wx,
    wy,
    kspace,
    grid,
    send_sem,
    recv_sem,
    side_send,
    side_recv,
):
    me = lax.axis_index("coil")
    frame = lax.axis_index("frame")
    after = lax.rem(frame + 1, frames)
    before = lax.rem(frame + frames - 1, frames)

    def peer_of(k):
        return lax.rem(me + k, coils)

    barrier = pltpu.get_barrier_semaphore()

    def greet(k, carry):
        pl.semaphore_signal(
            barrier, inc=1, device_id={"coil": peer_of(k)}, device_id_type=MESH
        )
        return carry

    lax.fori_loop(1, coils, greet, 0)
    for side in (after, before):
        pl.semaphore_signal(barrier, inc=1, device_id={"frame": side}, device_id_type=MESH)

    for part in range(2):
        current[0, part] = image_ref[:, part, :]

    def build(b, carry):
        row_taps = row_taps_ref[b].astype(F32)
        col_taps = col_taps_ref[b].astype(F32)
        wx[b] = taps_of(row_first_ref[pl.ds(b, 1), :], row_off_ref[0, b], row_taps)
        wy[b] = taps_of(col_first_ref[pl.ds(b, 1), :], col_off_ref[0, b], col_taps)
        return carry

    def to_all(phase, source, target):
        def copy_of(k):
            peer = peer_of(k)
            return pltpu.make_async_remote_copy(
                src_ref=source(peer),
                dst_ref=target(me),
                send_sem=send_sem.at[phase, k],
                recv_sem=recv_sem.at[phase, k],
                device_id={"coil": peer},
                device_id_type=MESH,
            )

        def start(k, carry):
            copy_of(k).start()
            return carry

        def arrive(k, carry):
            copy_of(k).wait_recv()
            return carry

        def leave(k, carry):
            copy_of(k).wait_send()
            return carry

        lax.fori_loop(1, coils, start, 0)
        return (
            lambda: lax.fori_loop(1, coils, arrive, 0),
            lambda: lax.fori_loop(1, coils, leave, 0),
        )

    pl.semaphore_wait(barrier, coils + 1)
    leaving = []
    for step in range(ITERS):
        low[step] = current[step].astype(BF16)
        arrived, left = to_all(
            2 * step, lambda peer: low.at[step], lambda own: gathered.at[step, own]
        )
        leaving.append(left)
        sides = []
        for slot, side in ((0, after), (1, before)):
            copy = pltpu.make_async_remote_copy(
                src_ref=current.at[step],
                dst_ref=beside.at[step, slot],
                send_sem=side_send.at[step, slot],
                recv_sem=side_recv.at[step, slot],
                device_id={"frame": side},
                device_id_type=MESH,
            )
            copy.start()
            sides.append(copy)
        gathered[step, me] = low[step]
        if step == 0:
            lax.fori_loop(0, NB, build, 0)
        arrived()

        cosine, sine, minus = table_ref[0], table_ref[1], table_ref[2]
        map_real = maps_ref[0].astype(F32)
        map_imag = maps_ref[1].astype(F32)
        image_real = gathered[step, :, 0].astype(F32).reshape(N, N)
        image_imag = gathered[step, :, 1].astype(F32).reshape(N, N)
        coil_real = (map_real * image_real - map_imag * image_imag).astype(BF16)
        coil_imag = (map_real * image_imag + map_imag * image_real).astype(BF16)
        half_real = (mm(cosine, coil_real) + mm(sine, coil_imag)).astype(BF16)
        half_imag = (mm(cosine, coil_imag) + mm(minus, coil_real)).astype(BF16)
        kspace[0:N] = (mm(half_real, cosine) + mm(half_imag, sine)).astype(BF16)
        kspace[N : 2 * N] = (mm(half_imag, cosine) + mm(half_real, minus)).astype(BF16)

        grid[...] = jnp.zeros_like(grid)

        def visit(b, misfit):
            across = mm(kspace[...], wy[b])
            rows = wx[b].astype(F32)
            measured = samples_ref[b].astype(F32)
            active = jnp.full((1, BS), b, jnp.int32) < used_ref[0]
            spread = []
            for part in range(2):
                predicted = jnp.sum(across[part * N : part * N + N] * rows, axis=0, keepdims=True)
                resid = jnp.where(active, predicted - measured[part : part + 1], 0.0)
                misfit = misfit + resid * resid
                spread.append((resid.astype(BF16).astype(F32) * rows).astype(BF16))
            grid[...] += mm_nt(jnp.concatenate(spread, axis=0), wy[b])
            return misfit

        misfit = lax.fori_loop(0, NB, visit, jnp.zeros((1, BS), F32))
        mis_out[step : step + 1, :] = misfit

        if step == ITERS - 1:
            all_misfit, left = to_all(
                2 * ITERS, lambda peer: mis_out, lambda own: mis_in.at[own]
            )
            leaving.append(left)
            mis_in[me] = mis_out[...]

        grid_real = grid[0:N].astype(BF16)
        grid_imag = grid[N : 2 * N].astype(BF16)
        back_real = (mm(cosine, grid_real) + mm(minus, grid_imag)).astype(BF16)
        back_imag = (mm(cosine, grid_imag) + mm(sine, grid_real)).astype(BF16)
        coil_real = mm(back_real, cosine) + mm(back_imag, minus)
        coil_imag = mm(back_imag, cosine) + mm(back_real, sine)
        height = N // coils
        part_out[step, :, 0] = (
            (map_real * coil_real + map_imag * coil_imag).reshape(coils, height, N).astype(BF16)
        )
        part_out[step, :, 1] = (
            (map_real * coil_imag - map_imag * coil_real).reshape(coils, height, N).astype(BF16)
        )
        arrived, left = to_all(
            2 * step + 1,
            lambda peer: part_out.at[step, peer],
            lambda own: part_in.at[step, own],
        )
        leaving.append(left)
        part_in[step, me] = part_out[step, me]
        for copy in sides:
            copy.wait()
        here = (current[step, 0], current[step, 1])
        early = (beside[step, 0, 0], beside[step, 0, 1])
        late = (beside[step, 1, 0], beside[step, 1, 1])
        first = slope(here, early)
        second = slope(late, here)
        arrived()
        result = []
        for part in range(2):
            gradient = jnp.sum(part_in[step, :, part].astype(F32), axis=0)
            result.append(
                here[part] - step_size * (gradient + tv_weight * (first[part] - second[part]))
            )
        result = wavelet_prox(result[0], result[1], step_size * shrink_weight)
        if step < ITERS - 1:
            for part in range(2):
                current[step + 1, part] = result[part]
        else:
            for part in range(2):
                out_ref[:, part, :] = result[part]

    all_misfit()
    total = jnp.sum(mis_in[...], axis=0)
    total = jnp.sum(total, axis=1, keepdims=True) * (0.5 / (coils * NB * BS))
    misfit_ref[...] = jnp.broadcast_to(total, misfit_ref.shape)
    for left in leaving:
        left()


def solution(mesh):
    coils = mesh.shape["coil"]
    frames = mesh.shape["frame"]
    height = N // coils
    tables = dft_tables()
    vmem = pl.BlockSpec(memory_space=pltpu.VMEM)
    smem = pl.BlockSpec(memory_space=pltpu.SMEM)

    def on_device(
        initial_image,
        coil_maps,
        samples,
        blocks_used,
        row_offset,
        col_offset,
        row_first,
        col_first,
        row_taps,
        col_taps,
    ):
        image, misfit = pl.pallas_call(
            functools.partial(kernel, coils, frames),
            out_shape=(
                jax.ShapeDtypeStruct((height, 2, N), F32),
                jax.ShapeDtypeStruct((ITERS, 128), F32),
            ),
            in_specs=[vmem, vmem, vmem, smem, smem, smem, vmem, vmem, vmem, vmem, vmem],
            out_specs=(vmem, vmem),
            scratch_shapes=[
                pltpu.VMEM((ITERS, 2, height, N), F32),
                pltpu.VMEM((ITERS, 2, height, N), BF16),
                pltpu.VMEM((ITERS, coils, 2, height, N), BF16),
                pltpu.VMEM((ITERS, 2, 2, height, N), F32),
                pltpu.VMEM((ITERS, coils, 2, height, N), BF16),
                pltpu.VMEM((ITERS, coils, 2, height, N), BF16),
                pltpu.VMEM((ITERS, BS), F32),
                pltpu.VMEM((coils, ITERS, BS), F32),
                pltpu.VMEM((NB, N, BS), BF16),
                pltpu.VMEM((NB, N, BS), BF16),
                pltpu.VMEM((2 * N, N), BF16),
                pltpu.VMEM((2 * N, N), F32),
                pltpu.SemaphoreType.DMA((2 * ITERS + 1, coils)),
                pltpu.SemaphoreType.DMA((2 * ITERS + 1, coils)),
                pltpu.SemaphoreType.DMA((ITERS, 2)),
                pltpu.SemaphoreType.DMA((ITERS, 2)),
            ],
            compiler_params=pltpu.CompilerParams(
                collective_id=0, has_side_effects=True, vmem_limit_bytes=40 * 1024 * 1024
            ),
        )(
            initial_image[:, 0],
            coil_maps[0],
            samples[0, 0],
            blocks_used,
            row_offset,
            col_offset,
            row_first[0],
            col_first[0],
            row_taps[0],
            col_taps[0],
            tables,
        )
        return image[:, None], misfit[:, :1]

    placed = (
        P("coil", "frame", None, None),
        P("coil", None, None, None),
        P("coil", "frame", None, None, None),
        P("frame"),
        P("frame", None),
        P("frame", None),
        P("frame", None, None),
        P("frame", None, None),
        P("frame", None, None, None),
        P("frame", None, None, None),
    )
    return jax.shard_map(
        on_device,
        mesh=mesh,
        in_specs=placed,
        out_specs=(P("coil", "frame", None, None), P(None, "frame")),
        check_vma=False,
    )
```

```python
import functools
import math

import jax
import jax.numpy as jnp
import numpy as np
from jax import lax
from jax.experimental import pallas as pl
from jax.experimental.pallas import tpu as pltpu
from jax.sharding import PartitionSpec as P

N = 256
NB = 18
BS = 256
KW = 4
ITERS = 2

step_size = 2.0
tv_weight = 0.1
smooth_floor = 0.5
shrink_weight = 0.1

RING = 8
RING_FAR = (4, 3, 5, 2, 6, 1, 7)
CROSS_FAR = (2, 1, 3)
GROUP = 6

MESH = pl.DeviceIdType.MESH
F32 = jnp.float32
BF16 = jnp.bfloat16


def dft_tables():
    counter = np.arange(N)
    angle = (counter[:, None] * counter[None, :] % N) * (2.0 * math.pi / N)
    cosine = jnp.asarray((np.cos(angle) / math.sqrt(N)).astype(np.float32)).astype(BF16)
    sine = jnp.asarray((np.sin(angle) / math.sqrt(N)).astype(np.float32)).astype(BF16)
    return np.stack([np.asarray(cosine), np.asarray(sine), np.asarray(-sine)])


def mm(a, b):
    return jnp.dot(a, b, preferred_element_type=F32)


def mm_nt(a, b):
    return lax.dot_general(a, b, (((1,), (1,)), ((), ())), preferred_element_type=F32)


def taps_of(first, offset, taps):
    distance = lax.broadcasted_iota(jnp.int32, (N, BS), 0) - (first + offset)
    matrix = jnp.zeros((N, BS), F32)
    for tap in range(KW):
        matrix = jnp.where(distance == tap, taps[tap : tap + 1, :], matrix)
    return matrix.astype(BF16)


def swap_lanes(field):
    lane = lax.broadcasted_iota(jnp.int32, field.shape, 1)
    width = field.shape[1]
    return jnp.where(
        lane % 2 == 0, pltpu.roll(field, width - 1, 1), pltpu.roll(field, 1, 1)
    )


def swap_rows(field):
    row = lax.broadcasted_iota(jnp.int32, field.shape, 0)
    height = field.shape[0]
    return jnp.where(
        row % 2 == 0, pltpu.roll(field, height - 1, 0), pltpu.roll(field, 1, 0)
    )


def shrunk(real, imag, limit):
    length = jnp.sqrt(real * real + imag * imag)
    factor = jnp.maximum(length - limit, 0.0) / jnp.maximum(length, limit)
    return real * factor, imag * factor


def wavelet_prox(real, imag, limit):
    parts = []
    for field in (real, imag):
        across = swap_lanes(field)
        down = swap_rows(field)
        both = swap_lanes(down)
        parts.append(
            (
                (field + across + down + both) * 0.5,
                (field - across + down - both) * 0.5,
                (field + across - down - both) * 0.5,
                (field - across - down + both) * 0.5,
            )
        )
    out_real, out_imag = parts[0][0], parts[1][0]
    for band in range(1, 4):
        band_real, band_imag = shrunk(parts[0][band], parts[1][band], limit)
        out_real = out_real + band_real
        out_imag = out_imag + band_imag
    return out_real * 0.5, out_imag * 0.5


def slope(late, early):
    real = late[0] - early[0]
    imag = late[1] - early[1]
    length = jnp.sqrt(real * real + imag * imag + smooth_floor * smooth_floor)
    return real / length, imag / length


def kernel(
    coils,
    frames,
    image_hbm,
    maps_hbm,
    samples_hbm,
    used_hbm,
    row_off_hbm,
    col_off_hbm,
    row_first_hbm,
    col_first_hbm,
    row_taps_hbm,
    col_taps_hbm,
    table_hbm,
    out_ref,
    misfit_ref,
    image_ref,
    maps_ref,
    samples_ref,
    used_ref,
    row_off_ref,
    col_off_ref,
    row_first_ref,
    col_first_ref,
    row_taps_ref,
    col_taps_ref,
    table_ref,
    current,
    low,
    gathered,
    beside,
    adjoint,
    part_out,
    part_in,
    mid_out,
    mid_in,
    mis_out,
    mis_in,
    mis_mid,
    mis_end,
    wx,
    wy,
    kspace,
    weighted,
    local_sem,
    ring_send,
    ring_recv,
    cross_send,
    cross_recv,
    side_send,
    side_recv,
    mis_send,
    mis_recv,
):
    me = lax.axis_index("coil")
    frame = lax.axis_index("frame")
    columns = coils // RING
    my_z = lax.rem(me, RING)
    my_x = me // RING
    height = N // coils

    def ring_coil(k):
        return my_x * RING + lax.rem(my_z + k, RING)

    def cross_x(k):
        return lax.rem(my_x + k, columns)

    def cross_coil(k):
        return cross_x(k) * RING + my_z

    after = lax.rem(frame + 1, frames)
    before = lax.rem(frame + frames - 1, frames)

    fetches = []
    for slot, (source, target) in enumerate(
        (
            (image_hbm, image_ref),
            (row_off_hbm, row_off_ref),
            (row_first_hbm, row_first_ref),
            (row_taps_hbm, row_taps_ref),
            (col_off_hbm, col_off_ref),
            (col_first_hbm, col_first_ref),
            (col_taps_hbm, col_taps_ref),
            (maps_hbm, maps_ref),
            (table_hbm, table_ref),
            (samples_hbm, samples_ref),
            (used_hbm, used_ref),
        )
    ):
        fetch = pltpu.make_async_copy(source, target, local_sem.at[slot])
        fetch.start()
        fetches.append(fetch)

    barrier = pltpu.get_barrier_semaphore()
    for k in RING_FAR:
        pl.semaphore_signal(
            barrier, inc=1, device_id={"coil": ring_coil(k)}, device_id_type=MESH
        )
    for k in CROSS_FAR:
        pl.semaphore_signal(
            barrier, inc=1, device_id={"coil": cross_coil(k)}, device_id_type=MESH
        )
    for side in (after, before):
        pl.semaphore_signal(barrier, inc=1, device_id={"frame": side}, device_id_type=MESH)

    leaving = []

    def send(source, target, send_sem, recv_sem, device):
        copy = pltpu.make_async_remote_copy(
            src_ref=source,
            dst_ref=target,
            send_sem=send_sem,
            recv_sem=recv_sem,
            device_id=device,
            device_id_type=MESH,
        )
        copy.start()
        leaving.append(copy)
        return copy

    fetches[0].wait()
    for part in range(2):
        current[0, part] = image_ref[:, part, :]
        low[0, part] = image_ref[:, part, :].astype(BF16)

    def build(first_ref, off_ref, taps_ref, out, b, carry):
        out[b] = taps_of(first_ref[b], off_ref[0, b], taps_ref[b].astype(F32))
        return carry

    for fetch in fetches[1:4]:
        fetch.wait()
    lax.fori_loop(
        0, NB, functools.partial(build, row_first_ref, row_off_ref, row_taps_ref, wx), 0
    )
    pl.semaphore_wait(barrier, RING - 1 + columns - 1 + 2)

    for step in range(ITERS):
        sides = [
            send(
                current.at[step],
                beside.at[step, slot],
                side_send.at[step, slot],
                side_recv.at[step, slot],
                {"frame": side},
            )
            for slot, side in ((0, after), (1, before))
        ]
        ring = {}
        cross = {}
        for k in RING_FAR:
            ring[k] = send(
                low.at[step],
                gathered.at[step, me],
                ring_send.at[2 * step, k],
                ring_recv.at[2 * step, k],
                {"coil": ring_coil(k)},
            )

        def forward(k, source):
            for far in CROSS_FAR:
                cross[far, k] = send(
                    source,
                    gathered.at[step, my_x * RING + lax.rem(my_z + RING - k, RING)],
                    cross_send.at[2 * step, far, k],
                    cross_recv.at[2 * step, far, k],
                    {"coil": cross_coil(far)},
                )

        forward(0, low.at[step])
        gathered[step, me] = low[step]
        if step == 0:
            for fetch in fetches[4:7]:
                fetch.wait()
            lax.fori_loop(
                0, NB, functools.partial(build, col_first_ref, col_off_ref, col_taps_ref, wy), 0
            )
            for fetch in fetches[7:]:
                fetch.wait()
        for k in reversed(RING_FAR):
            ring[k].wait_recv()
            forward(k, gathered.at[step, my_x * RING + lax.rem(my_z + RING - k, RING)])
        for copy in cross.values():
            copy.wait_recv()

        cosine, sine, minus = table_ref[0], table_ref[1], table_ref[2]
        map_real = maps_ref[0].astype(F32)
        map_imag = maps_ref[1].astype(F32)
        image_real = gathered[step, :, 0].astype(F32).reshape(N, N)
        image_imag = gathered[step, :, 1].astype(F32).reshape(N, N)
        coil_real = (map_real * image_real - map_imag * image_imag).astype(BF16)
        coil_imag = (map_real * image_imag + map_imag * image_real).astype(BF16)
        half_real = (mm(cosine, coil_real) + mm(sine, coil_imag)).astype(BF16)
        half_imag = (mm(cosine, coil_imag) + mm(minus, coil_real)).astype(BF16)
        kspace[0:N] = (mm(half_real, cosine) + mm(half_imag, sine)).astype(BF16)
        kspace[N : 2 * N] = (mm(half_imag, cosine) + mm(half_real, minus)).astype(BF16)

        def visit(b, misfit):
            across = mm(kspace[...], wy[b])
            rows = wx[b]
            wide = rows.astype(F32)
            measured = samples_ref[b].astype(F32)
            active = jnp.full((1, BS), b, jnp.int32) < used_ref[0]
            for part in range(2):
                predicted = jnp.sum(across[part * N : part * N + N] * wide, axis=0, keepdims=True)
                resid = jnp.where(active, predicted - measured[part : part + 1], 0.0)
                misfit = misfit + resid * resid
                weighted[b, part * N : part * N + N] = resid.astype(BF16) * rows
            return misfit

        def visits(group, misfit):
            for b in range(GROUP):
                misfit = visit(group * GROUP + b, misfit)
            return misfit

        misfit = lax.fori_loop(0, NB // GROUP, visits, jnp.zeros((1, BS), F32))
        mis_out[step : step + 1, :] = misfit

        if step == ITERS - 1:
            mis_cross = [
                send(
                    mis_out,
                    mis_in.at[far],
                    mis_send.at[0, far],
                    mis_recv.at[0, far],
                    {"coil": cross_coil(far)},
                )
                for far in CROSS_FAR
            ]

        total = mm_nt(weighted[0], wy[0])
        for b in range(1, NB):
            total = total + mm_nt(weighted[b], wy[b])
        grid_real = total[0:N].astype(BF16)
        grid_imag = total[N : 2 * N].astype(BF16)
        back_real = (mm(cosine, grid_real) + mm(minus, grid_imag)).astype(BF16)
        back_imag = (mm(cosine, grid_imag) + mm(sine, grid_real)).astype(BF16)
        coil_real = mm(back_real, cosine) + mm(back_imag, minus)
        coil_imag = mm(back_imag, cosine) + mm(back_real, sine)
        for part, field in enumerate(
            (
                map_real * coil_real + map_imag * coil_imag,
                map_real * coil_imag - map_imag * coil_real,
            )
        ):
            shards = field.reshape(coils, height, N)
            adjoint[:, part] = shards
            part_out[step, :, part] = shards.astype(BF16)

        cross = {}
        ring = {}
        for k in RING_FAR + (0,):
            for far in CROSS_FAR:
                cross[far, k] = send(
                    part_out.at[step, cross_x(far) * RING + lax.rem(my_z + k, RING)],
                    part_in.at[step, far, k],
                    cross_send.at[2 * step + 1, far, k],
                    cross_recv.at[2 * step + 1, far, k],
                    {"coil": cross_coil(far)},
                )
        if step == ITERS - 1:
            for copy in mis_cross:
                copy.wait_recv()
            mis_sum = mis_out[...]
            for far in CROSS_FAR:
                mis_sum = mis_sum + mis_in[far]
            mis_mid[...] = mis_sum
            mis_ring = [
                send(
                    mis_mid,
                    mis_end.at[k],
                    mis_send.at[1, k],
                    mis_recv.at[1, k],
                    {"coil": ring_coil(k)},
                )
                for k in RING_FAR
            ]
        for k in RING_FAR + (0,):
            pieces = adjoint[ring_coil(k)]
            for far in CROSS_FAR:
                cross[far, k].wait_recv()
                pieces = pieces + part_in[step, far, k].astype(F32)
            if k:
                mid_out[step, k] = pieces.astype(BF16)
                ring[k] = send(
                    mid_out.at[step, k],
                    mid_in.at[step, k],
                    ring_send.at[2 * step + 1, k],
                    ring_recv.at[2 * step + 1, k],
                    {"coil": ring_coil(k)},
                )
        for copy in sides:
            copy.wait_recv()
        here = (current[step, 0], current[step, 1])
        early = (beside[step, 0, 0], beside[step, 0, 1])
        late = (beside[step, 1, 0], beside[step, 1, 1])
        first = slope(here, early)
        second = slope(late, here)
        for k in RING_FAR:
            ring[k].wait_recv()
            pieces = pieces + mid_in[step, k].astype(F32)
        result = [
            here[part]
            - step_size * (pieces[part] + tv_weight * (first[part] - second[part]))
            for part in range(2)
        ]
        result = wavelet_prox(result[0], result[1], step_size * shrink_weight)
        for part in range(2):
            if step < ITERS - 1:
                current[step + 1, part] = result[part]
                low[step + 1, part] = result[part].astype(BF16)
            else:
                out_ref[:, part, :] = result[part]

    for copy in mis_ring:
        copy.wait_recv()
    for k in RING_FAR:
        mis_sum = mis_sum + mis_end[k]
    mis_sum = jnp.sum(mis_sum, axis=1, keepdims=True) * (0.5 / (coils * NB * BS))
    lane = lax.broadcasted_iota(jnp.int32, (1, ITERS), 1)
    misfit_ref[...] = jnp.where(lane == 0, mis_sum[0:1], mis_sum[1:2])
    for copy in leaving:
        copy.wait_send()


def solution(mesh):
    coils = mesh.shape["coil"]
    frames = mesh.shape["frame"]
    columns = coils // RING
    height = N // coils
    tables = dft_tables()
    vmem = pl.BlockSpec(memory_space=pltpu.VMEM)
    hbm = pl.BlockSpec(memory_space=pltpu.HBM)

    def on_device(
        initial_image,
        coil_maps,
        samples,
        blocks_used,
        row_offset,
        col_offset,
        row_first,
        col_first,
        row_taps,
        col_taps,
    ):
        image, misfit = pl.pallas_call(
            functools.partial(kernel, coils, frames),
            out_shape=(
                jax.ShapeDtypeStruct((height, 2, N), F32),
                jax.ShapeDtypeStruct((1, ITERS), F32),
            ),
            in_specs=[hbm] * 11,
            out_specs=(vmem, vmem),
            scratch_shapes=[
                pltpu.VMEM((height, 2, N), F32),
                pltpu.VMEM((2, N, N), BF16),
                pltpu.VMEM((NB, 2, BS), BF16),
                pltpu.SMEM((1,), jnp.int32),
                pltpu.SMEM((1, NB), jnp.int32),
                pltpu.SMEM((1, NB), jnp.int32),
                pltpu.VMEM((NB, 1, BS), jnp.int32),
                pltpu.VMEM((NB, 1, BS), jnp.int32),
                pltpu.VMEM((NB, KW, BS), BF16),
                pltpu.VMEM((NB, KW, BS), BF16),
                pltpu.VMEM((3, N, N), BF16),
                pltpu.VMEM((ITERS, 2, height, N), F32),
                pltpu.VMEM((ITERS, 2, height, N), BF16),
                pltpu.VMEM((ITERS, coils, 2, height, N), BF16),
                pltpu.VMEM((ITERS, 2, 2, height, N), F32),
                pltpu.VMEM((coils, 2, height, N), F32),
                pltpu.VMEM((ITERS, coils, 2, height, N), BF16),
                pltpu.VMEM((ITERS, columns, RING, 2, height, N), BF16),
                pltpu.VMEM((ITERS, RING, 2, height, N), BF16),
                pltpu.VMEM((ITERS, RING, 2, height, N), BF16),
                pltpu.VMEM((ITERS, BS), F32),
                pltpu.VMEM((columns, ITERS, BS), F32),
                pltpu.VMEM((ITERS, BS), F32),
                pltpu.VMEM((RING, ITERS, BS), F32),
                pltpu.VMEM((NB, N, BS), BF16),
                pltpu.VMEM((NB, N, BS), BF16),
                pltpu.VMEM((2 * N, N), BF16),
                pltpu.VMEM((NB, 2 * N, BS), BF16),
                pltpu.SemaphoreType.DMA((11,)),
                pltpu.SemaphoreType.DMA((2 * ITERS, RING)),
                pltpu.SemaphoreType.DMA((2 * ITERS, RING)),
                pltpu.SemaphoreType.DMA((2 * ITERS, columns, RING)),
                pltpu.SemaphoreType.DMA((2 * ITERS, columns, RING)),
                pltpu.SemaphoreType.DMA((ITERS, 2)),
                pltpu.SemaphoreType.DMA((ITERS, 2)),
                pltpu.SemaphoreType.DMA((2, RING)),
                pltpu.SemaphoreType.DMA((2, RING)),
            ],
            compiler_params=pltpu.CompilerParams(
                collective_id=0, has_side_effects=True, vmem_limit_bytes=67043328
            ),
        )(
            initial_image[:, 0],
            coil_maps[0],
            samples[0, 0],
            blocks_used,
            row_offset,
            col_offset,
            row_first[0][:, None],
            col_first[0][:, None],
            row_taps[0],
            col_taps[0],
            tables,
        )
        return image[:, None], misfit.T

    placed = (
        P("coil", "frame", None, None),
        P("coil", None, None, None),
        P("coil", "frame", None, None, None),
        P("frame"),
        P("frame", None),
        P("frame", None),
        P("frame", None, None),
        P("frame", None, None),
        P("frame", None, None, None),
        P("frame", None, None, None),
    )
    return jax.shard_map(
        on_device,
        mesh=mesh,
        in_specs=placed,
        out_specs=(P("coil", "frame", None, None), P(None, "frame")),
        check_vma=False,
    )
```

```python
import functools
import math

import jax
import jax.numpy as jnp
import numpy as np
from jax import lax
from jax.experimental import pallas as pl
from jax.experimental.pallas import tpu as pltpu
from jax.sharding import PartitionSpec as P

N = 256
NB = 18
BS = 256
KW = 4
ITERS = 2

step_size = 2.0
tv_weight = 0.1
smooth_floor = 0.5
shrink_weight = 0.1

RING = 8
RING_FAR = (4, 3, 5, 2, 6, 1, 7)
CROSS_FAR = (2, 1, 3)
ALL_FAR = sorted(
    ((far, k) for far in range(4) for k in range(RING) if far or k),
    key=lambda to: -(min(to[0], 4 - to[0]) + min(to[1], RING - to[1])),
)


MESH = pl.DeviceIdType.MESH
F32 = jnp.float32
BF16 = jnp.bfloat16


def dft_tables():
    counter = np.arange(N)
    angle = (counter[:, None] * counter[None, :] % N) * (2.0 * math.pi / N)
    cosine = jnp.asarray((np.cos(angle) / math.sqrt(N)).astype(np.float32)).astype(BF16)
    sine = jnp.asarray((np.sin(angle) / math.sqrt(N)).astype(np.float32)).astype(BF16)
    return np.stack([np.asarray(cosine), np.asarray(sine), np.asarray(-sine)])


def mm(a, b):
    return jnp.dot(a, b, preferred_element_type=F32)


def mm_nt(a, b):
    return lax.dot_general(a, b, (((1,), (1,)), ((), ())), preferred_element_type=F32)


def taps_of(first, offset, taps):
    distance = lax.broadcasted_iota(jnp.int32, (N, BS), 0) - (first + offset)
    matrix = jnp.zeros((N, BS), F32)
    for tap in range(KW):
        matrix = jnp.where(distance == tap, taps[tap : tap + 1, :], matrix)
    return matrix.astype(BF16)


def swap_lanes(field):
    lane = lax.broadcasted_iota(jnp.int32, field.shape, 1)
    width = field.shape[1]
    return jnp.where(
        lane % 2 == 0, pltpu.roll(field, width - 1, 1), pltpu.roll(field, 1, 1)
    )


def swap_rows(field):
    row = lax.broadcasted_iota(jnp.int32, field.shape, 0)
    height = field.shape[0]
    return jnp.where(
        row % 2 == 0, pltpu.roll(field, height - 1, 0), pltpu.roll(field, 1, 0)
    )


def shrunk(real, imag, limit):
    length = jnp.sqrt(real * real + imag * imag)
    factor = jnp.maximum(length - limit, 0.0) / jnp.maximum(length, limit)
    return real * factor, imag * factor


def wavelet_prox(real, imag, limit):
    parts = []
    for field in (real, imag):
        across = swap_lanes(field)
        down = swap_rows(field)
        both = swap_lanes(down)
        parts.append(
            (
                (field + across + down + both) * 0.5,
                (field - across + down - both) * 0.5,
                (field + across - down - both) * 0.5,
                (field - across - down + both) * 0.5,
            )
        )
    out_real, out_imag = parts[0][0], parts[1][0]
    for band in range(1, 4):
        band_real, band_imag = shrunk(parts[0][band], parts[1][band], limit)
        out_real = out_real + band_real
        out_imag = out_imag + band_imag
    return out_real * 0.5, out_imag * 0.5


def slope(late, early):
    real = late[0] - early[0]
    imag = late[1] - early[1]
    length = jnp.sqrt(real * real + imag * imag + smooth_floor * smooth_floor)
    return real / length, imag / length


def kernel(
    coils,
    frames,
    image_hbm,
    maps_hbm,
    samples_hbm,
    used_hbm,
    row_off_hbm,
    col_off_hbm,
    row_first_hbm,
    col_first_hbm,
    row_taps_hbm,
    col_taps_hbm,
    table_hbm,
    out_ref,
    misfit_ref,
    image_ref,
    maps_ref,
    samples_ref,
    used_ref,
    row_off_ref,
    col_off_ref,
    row_first_ref,
    col_first_ref,
    row_taps_ref,
    col_taps_ref,
    table_ref,
    current,
    low,
    gathered,
    beside,
    adjoint,
    part_out,
    part_in,
    mis_out,
    mis_in,
    wx,
    wy,
    kspace,
    weighted,
    back,
    local_sem,
    all_send,
    all_recv,
    side_send,
    side_recv,
):
    me = lax.axis_index("coil")
    frame = lax.axis_index("frame")
    columns = coils // RING
    my_z = lax.rem(me, RING)
    my_x = me // RING
    height = N // coils

    def ring_coil(k):
        return my_x * RING + lax.rem(my_z + k, RING)

    def cross_x(k):
        return lax.rem(my_x + k, columns)

    def cross_coil(k):
        return cross_x(k) * RING + my_z

    def any_coil(far, k):
        return cross_x(far) * RING + lax.rem(my_z + k, RING)

    after = lax.rem(frame + 1, frames)
    before = lax.rem(frame + frames - 1, frames)

    fetches = []
    for slot, (source, target) in enumerate(
        (
            (image_hbm, image_ref),
            (row_off_hbm, row_off_ref),
            (row_first_hbm, row_first_ref),
            (row_taps_hbm, row_taps_ref),
            (col_off_hbm, col_off_ref),
            (col_first_hbm, col_first_ref),
            (col_taps_hbm, col_taps_ref),
            (maps_hbm, maps_ref),
            (table_hbm, table_ref),
            (samples_hbm, samples_ref),
            (used_hbm, used_ref),
        )
    ):
        fetch = pltpu.make_async_copy(source, target, local_sem.at[slot])
        fetch.start()
        fetches.append(fetch)

    barrier = pltpu.get_barrier_semaphore()
    for k in RING_FAR:
        pl.semaphore_signal(
            barrier, inc=1, device_id={"coil": ring_coil(k)}, device_id_type=MESH
        )
    for k in CROSS_FAR:
        pl.semaphore_signal(
            barrier, inc=1, device_id={"coil": cross_coil(k)}, device_id_type=MESH
        )
    for side in (after, before):
        pl.semaphore_signal(barrier, inc=1, device_id={"frame": side}, device_id_type=MESH)

    leaving = []

    def send(source, target, send_sem, recv_sem, device):
        copy = pltpu.make_async_remote_copy(
            src_ref=source,
            dst_ref=target,
            send_sem=send_sem,
            recv_sem=recv_sem,
            device_id=device,
            device_id_type=MESH,
        )
        copy.start()
        leaving.append(copy)
        return copy

    fetches[0].wait()
    for part in range(2):
        current[0, part] = image_ref[:, part, :]
        low[0, part] = image_ref[:, part, :].astype(BF16)

    def build(first_ref, off_ref, taps_ref, out, b, carry):
        out[b] = taps_of(first_ref[b], off_ref[0, b], taps_ref[b].astype(F32))
        return carry

    def build_rows(start, stop):
        lax.fori_loop(
            start, stop, functools.partial(build, row_first_ref, row_off_ref, row_taps_ref, wx), 0
        )

    def build_columns(start, stop):
        lax.fori_loop(
            start, stop, functools.partial(build, col_first_ref, col_off_ref, col_taps_ref, wy), 0
        )

    pl.semaphore_wait(barrier, RING - 1 + columns - 1 + 2)

    for step in range(ITERS):
        sides = [
            send(
                current.at[step],
                beside.at[step, slot],
                side_send.at[step, slot],
                side_recv.at[step, slot],
                {"frame": side},
            )
            for slot, side in ((0, after), (1, before))
        ]
        gathered[step, me] = low[step]
        if step == 0:
            ring = {}
            cross = []
            for k in RING_FAR:
                ring[k] = send(
                    low.at[step],
                    gathered.at[step, me],
                    all_send.at[2 * step, 0, k],
                    all_recv.at[2 * step, 0, k],
                    {"coil": ring_coil(k)},
                )

            def forward(k, source):
                for far in CROSS_FAR:
                    copy = send(
                        source,
                        gathered.at[step, ring_coil(RING - k)],
                        all_send.at[2 * step, far, k],
                        all_recv.at[2 * step, far, k],
                        {"coil": cross_coil(far)},
                    )
                    cross.append(copy)

            forward(0, low.at[step])
            for fetch in fetches[1:7]:
                fetch.wait()
            build_rows(0, NB)
            build_columns(0, NB // 3)
            for k in reversed(RING_FAR):
                if k == 6:
                    build_columns(NB // 3, NB - NB // 3)
                if k == 5:
                    build_columns(NB - NB // 3, NB)
                ring[k].wait_recv()
                forward(k, gathered.at[step, ring_coil(RING - k)])
            for fetch in fetches[7:]:
                fetch.wait()
            for copy in cross:
                copy.wait_recv()
        else:
            copies = [
                send(
                    low.at[step],
                    gathered.at[step, me],
                    all_send.at[2 * step, far, k],
                    all_recv.at[2 * step, far, k],
                    {"coil": any_coil(far, k)},
                )
                for far, k in ALL_FAR
            ]
            for copy in copies:
                copy.wait_recv()

        cosine, sine, minus = table_ref[0], table_ref[1], table_ref[2]
        map_real = maps_ref[0].astype(F32)
        map_imag = maps_ref[1].astype(F32)
        image_real = gathered[step, :, 0].astype(F32).reshape(N, N)
        image_imag = gathered[step, :, 1].astype(F32).reshape(N, N)
        coil_real = (map_real * image_real - map_imag * image_imag).astype(BF16)
        coil_imag = (map_real * image_imag + map_imag * image_real).astype(BF16)
        half_real = (mm(cosine, coil_real) + mm(sine, coil_imag)).astype(BF16)
        half_imag = (mm(cosine, coil_imag) + mm(minus, coil_real)).astype(BF16)
        kspace[0:N] = (mm(half_real, cosine) + mm(half_imag, sine)).astype(BF16)
        kspace[N : 2 * N] = (mm(half_imag, cosine) + mm(half_real, minus)).astype(BF16)

        def visit(b, misfit):
            rows = wx[b]
            wide = rows.astype(F32)
            measured = samples_ref[b].astype(F32)
            active = jnp.full((1, BS), b, jnp.int32) < used_ref[0]
            for part in range(2):
                across = mm(kspace[part * N : part * N + N], wy[b])
                predicted = jnp.sum(across * wide, axis=0, keepdims=True)
                resid = jnp.where(active, predicted - measured[part : part + 1], 0.0)
                misfit = misfit + resid * resid
                weighted[b, part * N : part * N + N] = resid.astype(BF16) * rows
            return misfit

        misfit = jnp.zeros((1, BS), F32)
        for b in range(NB):
            misfit = visit(b, misfit)
        mis_out[step : step + 1, :] = misfit

        if step == ITERS - 1:
            mis_copies = [
                send(
                    mis_out,
                    mis_in.at[far, k],
                    all_send.at[2 * ITERS, far, k],
                    all_recv.at[2 * ITERS, far, k],
                    {"coil": any_coil(far, k)},
                )
                for far, k in ALL_FAR
            ]

        totals = []
        for part in range(2):
            total = mm_nt(weighted[0, part * N : part * N + N], wy[0])
            for b in range(1, NB):
                total = total + mm_nt(weighted[b, part * N : part * N + N], wy[b])
            totals.append(total.astype(BF16))
        grid_real, grid_imag = totals
        back[0] = (mm(cosine, grid_real) + mm(minus, grid_imag)).astype(BF16)
        back[1] = (mm(cosine, grid_imag) + mm(sine, grid_real)).astype(BF16)
        copies = []
        for far in CROSS_FAR + (0,):
            strip = pl.ds(pl.multiple_of(cross_x(far) * RING * height, RING * height), RING * height)
            back_real, back_imag = back[0, strip], back[1, strip]
            map_real = maps_ref[0, strip].astype(F32)
            map_imag = maps_ref[1, strip].astype(F32)
            coil_real = mm(back_real, cosine) + mm(back_imag, minus)
            coil_imag = mm(back_imag, cosine) + mm(back_real, sine)
            for part, field in enumerate(
                (
                    map_real * coil_real + map_imag * coil_imag,
                    map_real * coil_imag - map_imag * coil_real,
                )
            ):
                shards = field.reshape(RING, height, N)
                part_out[step, far, :, part] = shards.astype(BF16)
                if far == 0:
                    adjoint[:, part] = shards
            for k in RING_FAR + (0,):
                if far or k:
                    copies.append(
                        send(
                            part_out.at[step, far, lax.rem(my_z + k, RING)],
                            part_in.at[step, far, k],
                            all_send.at[2 * step + 1, far, k],
                            all_recv.at[2 * step + 1, far, k],
                            {"coil": any_coil(far, k)},
                        )
                    )

        for copy in sides:
            copy.wait_recv()
        here = (current[step, 0], current[step, 1])
        early = (beside[step, 0, 0], beside[step, 0, 1])
        late = (beside[step, 1, 0], beside[step, 1, 1])
        first = slope(here, early)
        second = slope(late, here)
        pieces = adjoint[my_z]
        for copy in copies:
            copy.wait_recv()
        for far in range(columns):
            for k in range(RING):
                if far or k:
                    pieces = pieces + part_in[step, far, k].astype(F32)
        result = [
            here[part]
            - step_size * (pieces[part] + tv_weight * (first[part] - second[part]))
            for part in range(2)
        ]
        result = wavelet_prox(result[0], result[1], step_size * shrink_weight)
        for part in range(2):
            if step < ITERS - 1:
                current[step + 1, part] = result[part]
                low[step + 1, part] = result[part].astype(BF16)
            else:
                out_ref[:, part, :] = result[part]

    mis_sum = mis_out[...]
    for copy in mis_copies:
        copy.wait_recv()
    for far, k in ALL_FAR:
        mis_sum = mis_sum + mis_in[far, k]
    mis_sum = jnp.sum(mis_sum, axis=1, keepdims=True) * (0.5 / (coils * NB * BS))
    lane = lax.broadcasted_iota(jnp.int32, (1, ITERS), 1)
    misfit_ref[...] = jnp.where(lane == 0, mis_sum[0:1], mis_sum[1:2])
    for copy in leaving:
        copy.wait_send()


def solution(mesh):
    coils = mesh.shape["coil"]
    frames = mesh.shape["frame"]
    columns = coils // RING
    height = N // coils
    tables = dft_tables()
    vmem = pl.BlockSpec(memory_space=pltpu.VMEM)
    hbm = pl.BlockSpec(memory_space=pltpu.HBM)

    def on_device(
        initial_image,
        coil_maps,
        samples,
        blocks_used,
        row_offset,
        col_offset,
        row_first,
        col_first,
        row_taps,
        col_taps,
    ):
        image, misfit = pl.pallas_call(
            functools.partial(kernel, coils, frames),
            out_shape=(
                jax.ShapeDtypeStruct((height, 2, N), F32),
                jax.ShapeDtypeStruct((1, ITERS), F32),
            ),
            in_specs=[hbm] * 11,
            out_specs=(vmem, vmem),
            scratch_shapes=[
                pltpu.VMEM((height, 2, N), F32),
                pltpu.VMEM((2, N, N), BF16),
                pltpu.VMEM((NB, 2, BS), BF16),
                pltpu.SMEM((1,), jnp.int32),
                pltpu.SMEM((1, NB), jnp.int32),
                pltpu.SMEM((1, NB), jnp.int32),
                pltpu.VMEM((NB, 1, BS), jnp.int32),
                pltpu.VMEM((NB, 1, BS), jnp.int32),
                pltpu.VMEM((NB, KW, BS), BF16),
                pltpu.VMEM((NB, KW, BS), BF16),
                pltpu.VMEM((3, N, N), BF16),
                pltpu.VMEM((ITERS, 2, height, N), F32),
                pltpu.VMEM((ITERS, 2, height, N), BF16),
                pltpu.VMEM((ITERS, coils, 2, height, N), BF16),
                pltpu.VMEM((ITERS, 2, 2, height, N), F32),
                pltpu.VMEM((RING, 2, height, N), F32),
                pltpu.VMEM((ITERS, columns, RING, 2, height, N), BF16),
                pltpu.VMEM((ITERS, columns, RING, 2, height, N), BF16),
                pltpu.VMEM((ITERS, BS), F32),
                pltpu.VMEM((columns, RING, ITERS, BS), F32),
                pltpu.VMEM((NB, N, BS), BF16),
                pltpu.VMEM((NB, N, BS), BF16),
                pltpu.VMEM((2 * N, N), BF16),
                pltpu.VMEM((NB, 2 * N, BS), BF16),
                pltpu.VMEM((2, N, N), BF16),
                pltpu.SemaphoreType.DMA((11,)),
                pltpu.SemaphoreType.DMA((2 * ITERS + 1, columns, RING)),
                pltpu.SemaphoreType.DMA((2 * ITERS + 1, columns, RING)),
                pltpu.SemaphoreType.DMA((ITERS, 2)),
                pltpu.SemaphoreType.DMA((ITERS, 2)),
            ],
            compiler_params=pltpu.CompilerParams(
                collective_id=0, has_side_effects=True, vmem_limit_bytes=67043328
            ),
        )(
            initial_image[:, 0],
            coil_maps[0],
            samples[0, 0],
            blocks_used,
            row_offset,
            col_offset,
            row_first[0][:, None],
            col_first[0][:, None],
            row_taps[0],
            col_taps[0],
            tables,
        )
        return image[:, None], misfit.T

    placed = (
        P("coil", "frame", None, None),
        P("coil", None, None, None),
        P("coil", "frame", None, None, None),
        P("frame"),
        P("frame", None),
        P("frame", None),
        P("frame", None, None),
        P("frame", None, None),
        P("frame", None, None, None),
        P("frame", None, None, None),
    )
    return jax.shard_map(
        on_device,
        mesh=mesh,
        in_specs=placed,
        out_specs=(P("coil", "frame", None, None), P(None, "frame")),
        check_vma=False,
    )
```

```python
import functools
import math

import jax
import jax.numpy as jnp
import numpy as np
from jax import lax
from jax.experimental import pallas as pl
from jax.experimental.pallas import tpu as pltpu
from jax.sharding import PartitionSpec as P

N = 256
NB = 18
BS = 256
KW = 4
ITERS = 2

step_size = 2.0
tv_weight = 0.1
smooth_floor = 0.5
shrink_weight = 0.1

RING = 8
RING_FAR = (4, 3, 5, 2, 6, 1, 7)
CROSS_FAR = (2, 1, 3)
ALL_FAR = sorted(
    ((far, k) for far in range(4) for k in range(RING) if far or k),
    key=lambda to: -(min(to[0], 4 - to[0]) + min(to[1], RING - to[1])),
)


MESH = pl.DeviceIdType.MESH
F32 = jnp.float32
BF16 = jnp.bfloat16


def dft_tables():
    counter = np.arange(N)
    angle = (counter[:, None] * counter[None, :] % N) * (2.0 * math.pi / N)
    cosine = jnp.asarray((np.cos(angle) / math.sqrt(N)).astype(np.float32)).astype(BF16)
    sine = jnp.asarray((np.sin(angle) / math.sqrt(N)).astype(np.float32)).astype(BF16)
    return np.stack([np.asarray(cosine), np.asarray(sine), np.asarray(-sine)])


def mm(a, b):
    return jnp.dot(a, b, preferred_element_type=F32)


def mm_nt(a, b):
    return lax.dot_general(a, b, (((1,), (1,)), ((), ())), preferred_element_type=F32)


def taps_of(first, offset, taps):
    distance = lax.broadcasted_iota(jnp.int32, (N, BS), 0) - (first + offset)
    matrix = jnp.zeros((N, BS), F32)
    for tap in range(KW):
        matrix = jnp.where(distance == tap, taps[tap : tap + 1, :], matrix)
    return matrix.astype(BF16)


def swap_lanes(field):
    lane = lax.broadcasted_iota(jnp.int32, field.shape, 1)
    width = field.shape[1]
    return jnp.where(
        lane % 2 == 0, pltpu.roll(field, width - 1, 1), pltpu.roll(field, 1, 1)
    )


def swap_rows(field):
    row = lax.broadcasted_iota(jnp.int32, field.shape, 0)
    height = field.shape[0]
    return jnp.where(
        row % 2 == 0, pltpu.roll(field, height - 1, 0), pltpu.roll(field, 1, 0)
    )


def shrunk(real, imag, limit):
    length = jnp.sqrt(real * real + imag * imag)
    factor = jnp.maximum(length - limit, 0.0) / jnp.maximum(length, limit)
    return real * factor, imag * factor


def wavelet_prox(real, imag, limit):
    parts = []
    for field in (real, imag):
        across = swap_lanes(field)
        down = swap_rows(field)
        both = swap_lanes(down)
        parts.append(
            (
                (field + across + down + both) * 0.5,
                (field - across + down - both) * 0.5,
                (field + across - down - both) * 0.5,
                (field - across - down + both) * 0.5,
            )
        )
    out_real, out_imag = parts[0][0], parts[1][0]
    for band in range(1, 4):
        band_real, band_imag = shrunk(parts[0][band], parts[1][band], limit)
        out_real = out_real + band_real
        out_imag = out_imag + band_imag
    return out_real * 0.5, out_imag * 0.5


def slope(late, early):
    real = late[0] - early[0]
    imag = late[1] - early[1]
    length = jnp.sqrt(real * real + imag * imag + smooth_floor * smooth_floor)
    return real / length, imag / length


def kernel(
    coils,
    frames,
    image_hbm,
    maps_hbm,
    samples_hbm,
    used_hbm,
    row_off_hbm,
    col_off_hbm,
    row_first_hbm,
    col_first_hbm,
    row_taps_hbm,
    col_taps_hbm,
    table_hbm,
    out_ref,
    misfit_ref,
    image_ref,
    maps_ref,
    samples_ref,
    used_ref,
    row_off_ref,
    col_off_ref,
    row_first_ref,
    col_first_ref,
    row_taps_ref,
    col_taps_ref,
    table_ref,
    current,
    low,
    gathered,
    beside,
    adjoint,
    part_out,
    part_in,
    mis_out,
    mis_in,
    mis_mid,
    mis_end,
    wx,
    wy,
    kspace,
    weighted,
    back,
    local_sem,
    all_send,
    all_recv,
    side_send,
    side_recv,
    mis_send,
    mis_recv,
):
    me = lax.axis_index("coil")
    frame = lax.axis_index("frame")
    columns = coils // RING
    my_z = lax.rem(me, RING)
    my_x = me // RING
    height = N // coils

    def ring_coil(k):
        return my_x * RING + lax.rem(my_z + k, RING)

    def cross_x(k):
        return lax.rem(my_x + k, columns)

    def cross_coil(k):
        return cross_x(k) * RING + my_z

    def any_coil(far, k):
        return cross_x(far) * RING + lax.rem(my_z + k, RING)

    after = lax.rem(frame + 1, frames)
    before = lax.rem(frame + frames - 1, frames)

    fetches = []
    for slot, (source, target) in enumerate(
        (
            (image_hbm, image_ref),
            (row_off_hbm, row_off_ref),
            (row_first_hbm, row_first_ref),
            (row_taps_hbm, row_taps_ref),
            (col_off_hbm, col_off_ref),
            (col_first_hbm, col_first_ref),
            (col_taps_hbm, col_taps_ref),
            (maps_hbm, maps_ref),
            (table_hbm, table_ref),
            (samples_hbm, samples_ref),
            (used_hbm, used_ref),
        )
    ):
        fetch = pltpu.make_async_copy(source, target, local_sem.at[slot])
        fetch.start()
        fetches.append(fetch)

    barrier = pltpu.get_barrier_semaphore()
    for k in RING_FAR:
        pl.semaphore_signal(
            barrier, inc=1, device_id={"coil": ring_coil(k)}, device_id_type=MESH
        )
    for k in CROSS_FAR:
        pl.semaphore_signal(
            barrier, inc=1, device_id={"coil": cross_coil(k)}, device_id_type=MESH
        )
    for side in (after, before):
        pl.semaphore_signal(barrier, inc=1, device_id={"frame": side}, device_id_type=MESH)

    leaving = []

    def send(source, target, send_sem, recv_sem, device):
        copy = pltpu.make_async_remote_copy(
            src_ref=source,
            dst_ref=target,
            send_sem=send_sem,
            recv_sem=recv_sem,
            device_id=device,
            device_id_type=MESH,
        )
        copy.start()
        leaving.append(copy)
        return copy

    fetches[0].wait()
    for part in range(2):
        current[0, part] = image_ref[:, part, :]
        low[0, part] = image_ref[:, part, :].astype(BF16)

    def build(first_ref, off_ref, taps_ref, out, b, carry):
        out[b] = taps_of(first_ref[b], off_ref[0, b], taps_ref[b].astype(F32))
        return carry

    def build_rows(start, stop):
        lax.fori_loop(
            start, stop, functools.partial(build, row_first_ref, row_off_ref, row_taps_ref, wx), 0
        )

    def build_columns(start, stop):
        lax.fori_loop(
            start, stop, functools.partial(build, col_first_ref, col_off_ref, col_taps_ref, wy), 0
        )

    pl.semaphore_wait(barrier, RING - 1 + columns - 1 + 2)

    for step in range(ITERS):
        sides = [
            send(
                current.at[step],
                beside.at[step, slot],
                side_send.at[step, slot],
                side_recv.at[step, slot],
                {"frame": side},
            )
            for slot, side in ((0, after), (1, before))
        ]
        gathered[step, me] = low[step]
        if step == 0:
            ring = {}
            cross = []
            for k in RING_FAR:
                ring[k] = send(
                    low.at[step],
                    gathered.at[step, me],
                    all_send.at[2 * step, 0, k],
                    all_recv.at[2 * step, 0, k],
                    {"coil": ring_coil(k)},
                )

            def forward(k, source):
                for far in CROSS_FAR:
                    copy = send(
                        source,
                        gathered.at[step, ring_coil(RING - k)],
                        all_send.at[2 * step, far, k],
                        all_recv.at[2 * step, far, k],
                        {"coil": cross_coil(far)},
                    )
                    cross.append(copy)

            forward(0, low.at[step])
            for fetch in fetches[1:7]:
                fetch.wait()
            build_rows(0, NB)
            build_columns(0, NB // 3)
            for k in reversed(RING_FAR):
                if k == 6:
                    build_columns(NB // 3, NB - NB // 3)
                if k == 5:
                    build_columns(NB - NB // 3, NB)
                ring[k].wait_recv()
                forward(k, gathered.at[step, ring_coil(RING - k)])
            for fetch in fetches[7:]:
                fetch.wait()
            for copy in cross:
                copy.wait_recv()
        else:
            copies = [
                send(
                    low.at[step],
                    gathered.at[step, me],
                    all_send.at[2 * step, far, k],
                    all_recv.at[2 * step, far, k],
                    {"coil": any_coil(far, k)},
                )
                for far, k in ALL_FAR
            ]
            for copy in copies:
                copy.wait_recv()

        cosine, sine, minus = table_ref[0], table_ref[1], table_ref[2]
        map_real = maps_ref[0].astype(F32)
        map_imag = maps_ref[1].astype(F32)
        image_real = gathered[step, :, 0].astype(F32).reshape(N, N)
        image_imag = gathered[step, :, 1].astype(F32).reshape(N, N)
        coil_real = (map_real * image_real - map_imag * image_imag).astype(BF16)
        coil_imag = (map_real * image_imag + map_imag * image_real).astype(BF16)
        half_real = (mm(cosine, coil_real) + mm(sine, coil_imag)).astype(BF16)
        half_imag = (mm(cosine, coil_imag) + mm(minus, coil_real)).astype(BF16)
        kspace[0:N] = (mm(half_real, cosine) + mm(half_imag, sine)).astype(BF16)
        kspace[N : 2 * N] = (mm(half_imag, cosine) + mm(half_real, minus)).astype(BF16)

        def visit(b, misfit):
            rows = wx[b]
            wide = rows.astype(F32)
            measured = samples_ref[b].astype(F32)
            active = jnp.full((1, BS), b, jnp.int32) < used_ref[0]
            for part in range(2):
                across = mm(kspace[part * N : part * N + N], wy[b])
                predicted = jnp.sum(across * wide, axis=0, keepdims=True)
                resid = jnp.where(active, predicted - measured[part : part + 1], 0.0)
                misfit = misfit + resid * resid
                weighted[b, part * N : part * N + N] = resid.astype(BF16) * rows
            return misfit

        misfit = jnp.zeros((1, BS), F32)
        for b in range(NB):
            misfit = visit(b, misfit)
        mis_out[step : step + 1, :] = misfit

        if step == ITERS - 1:
            mis_cross = [
                send(
                    mis_out,
                    mis_in.at[far],
                    mis_send.at[0, far],
                    mis_recv.at[0, far],
                    {"coil": cross_coil(far)},
                )
                for far in CROSS_FAR
            ]

        totals = []
        for part in range(2):
            total = mm_nt(weighted[0, part * N : part * N + N], wy[0])
            for b in range(1, NB):
                total = total + mm_nt(weighted[b, part * N : part * N + N], wy[b])
            totals.append(total.astype(BF16))
        grid_real, grid_imag = totals
        back[0] = (mm(cosine, grid_real) + mm(minus, grid_imag)).astype(BF16)
        back[1] = (mm(cosine, grid_imag) + mm(sine, grid_real)).astype(BF16)
        copies = []
        for far in CROSS_FAR + (0,):
            strip = pl.ds(pl.multiple_of(cross_x(far) * RING * height, RING * height), RING * height)
            back_real, back_imag = back[0, strip], back[1, strip]
            map_real = maps_ref[0, strip].astype(F32)
            map_imag = maps_ref[1, strip].astype(F32)
            coil_real = mm(back_real, cosine) + mm(back_imag, minus)
            coil_imag = mm(back_imag, cosine) + mm(back_real, sine)
            for part, field in enumerate(
                (
                    map_real * coil_real + map_imag * coil_imag,
                    map_real * coil_imag - map_imag * coil_real,
                )
            ):
                shards = field.reshape(RING, height, N)
                part_out[step, far, :, part] = shards.astype(BF16)
                if far == 0:
                    adjoint[:, part] = shards
            for k in RING_FAR + (0,):
                if far or k:
                    copies.append(
                        send(
                            part_out.at[step, far, lax.rem(my_z + k, RING)],
                            part_in.at[step, far, k],
                            all_send.at[2 * step + 1, far, k],
                            all_recv.at[2 * step + 1, far, k],
                            {"coil": any_coil(far, k)},
                        )
                    )

        if step == ITERS - 1:
            for copy in mis_cross:
                copy.wait_recv()
            mis_sum = mis_out[...]
            for far in CROSS_FAR:
                mis_sum = mis_sum + mis_in[far]
            mis_mid[...] = mis_sum
            mis_ring = [
                send(
                    mis_mid,
                    mis_end.at[k],
                    mis_send.at[1, k],
                    mis_recv.at[1, k],
                    {"coil": ring_coil(k)},
                )
                for k in RING_FAR
            ]
        for copy in sides:
            copy.wait_recv()
        here = (current[step, 0], current[step, 1])
        early = (beside[step, 0, 0], beside[step, 0, 1])
        late = (beside[step, 1, 0], beside[step, 1, 1])
        first = slope(here, early)
        second = slope(late, here)
        pieces = adjoint[my_z]
        for copy in copies:
            copy.wait_recv()
        for far in range(columns):
            for k in range(RING):
                if far or k:
                    pieces = pieces + part_in[step, far, k].astype(F32)
        result = [
            here[part]
            - step_size * (pieces[part] + tv_weight * (first[part] - second[part]))
            for part in range(2)
        ]
        result = wavelet_prox(result[0], result[1], step_size * shrink_weight)
        for part in range(2):
            if step < ITERS - 1:
                current[step + 1, part] = result[part]
                low[step + 1, part] = result[part].astype(BF16)
            else:
                out_ref[:, part, :] = result[part]

    for copy in mis_ring:
        copy.wait_recv()
    for k in RING_FAR:
        mis_sum = mis_sum + mis_end[k]
    mis_sum = jnp.sum(mis_sum, axis=1, keepdims=True) * (0.5 / (coils * NB * BS))
    lane = lax.broadcasted_iota(jnp.int32, (1, ITERS), 1)
    misfit_ref[...] = jnp.where(lane == 0, mis_sum[0:1], mis_sum[1:2])
    for copy in leaving:
        copy.wait_send()


def solution(mesh):
    coils = mesh.shape["coil"]
    frames = mesh.shape["frame"]
    columns = coils // RING
    height = N // coils
    tables = dft_tables()
    vmem = pl.BlockSpec(memory_space=pltpu.VMEM)
    hbm = pl.BlockSpec(memory_space=pltpu.HBM)

    def on_device(
        initial_image,
        coil_maps,
        samples,
        blocks_used,
        row_offset,
        col_offset,
        row_first,
        col_first,
        row_taps,
        col_taps,
    ):
        image, misfit = pl.pallas_call(
            functools.partial(kernel, coils, frames),
            out_shape=(
                pltpu.VMEM((height, 2, N), F32),
                pltpu.VMEM((1, ITERS), F32),
            ),
            in_specs=[hbm] * 11,
            out_specs=(vmem, vmem),
            scratch_shapes=[
                pltpu.VMEM((height, 2, N), F32),
                pltpu.VMEM((2, N, N), BF16),
                pltpu.VMEM((NB, 2, BS), BF16),
                pltpu.SMEM((1,), jnp.int32),
                pltpu.SMEM((1, NB), jnp.int32),
                pltpu.SMEM((1, NB), jnp.int32),
                pltpu.VMEM((NB, 1, BS), jnp.int32),
                pltpu.VMEM((NB, 1, BS), jnp.int32),
                pltpu.VMEM((NB, KW, BS), BF16),
                pltpu.VMEM((NB, KW, BS), BF16),
                pltpu.VMEM((3, N, N), BF16),
                pltpu.VMEM((ITERS, 2, height, N), F32),
                pltpu.VMEM((ITERS, 2, height, N), BF16),
                pltpu.VMEM((ITERS, coils, 2, height, N), BF16),
                pltpu.VMEM((ITERS, 2, 2, height, N), F32),
                pltpu.VMEM((RING, 2, height, N), F32),
                pltpu.VMEM((ITERS, columns, RING, 2, height, N), BF16),
                pltpu.VMEM((ITERS, columns, RING, 2, height, N), BF16),
                pltpu.VMEM((ITERS, BS), F32),
                pltpu.VMEM((columns, ITERS, BS), F32),
                pltpu.VMEM((ITERS, BS), F32),
                pltpu.VMEM((RING, ITERS, BS), F32),
                pltpu.VMEM((NB, N, BS), BF16),
                pltpu.VMEM((NB, N, BS), BF16),
                pltpu.VMEM((2 * N, N), BF16),
                pltpu.VMEM((NB, 2 * N, BS), BF16),
                pltpu.VMEM((2, N, N), BF16),
                pltpu.SemaphoreType.DMA((11,)),
                pltpu.SemaphoreType.DMA((2 * ITERS, columns, RING)),
                pltpu.SemaphoreType.DMA((2 * ITERS, columns, RING)),
                pltpu.SemaphoreType.DMA((ITERS, 2)),
                pltpu.SemaphoreType.DMA((ITERS, 2)),
                pltpu.SemaphoreType.DMA((2, RING)),
                pltpu.SemaphoreType.DMA((2, RING)),
            ],
            compiler_params=pltpu.CompilerParams(
                collective_id=0, has_side_effects=True, vmem_limit_bytes=67043328 - 32 * 1024
            ),
        )(
            initial_image[:, 0],
            coil_maps[0],
            samples[0, 0],
            blocks_used,
            row_offset,
            col_offset,
            row_first[0][:, None],
            col_first[0][:, None],
            row_taps[0],
            col_taps[0],
            tables,
        )
        return image[:, None], misfit.T

    placed = (
        P("coil", "frame", None, None),
        P("coil", None, None, None),
        P("coil", "frame", None, None, None),
        P("frame"),
        P("frame", None),
        P("frame", None),
        P("frame", None, None),
        P("frame", None, None),
        P("frame", None, None, None),
        P("frame", None, None, None),
    )
    return jax.shard_map(
        on_device,
        mesh=mesh,
        in_specs=placed,
        out_specs=(P("coil", "frame", None, None), P(None, "frame")),
        check_vma=False,
    )
```

```python
import functools
import math

import jax
import jax.numpy as jnp
import numpy as np
from jax import lax
from jax.experimental import pallas as pl
from jax.experimental.pallas import tpu as pltpu
from jax.sharding import PartitionSpec as P

N = 256
NB = 18
BS = 256
KW = 4
ITERS = 2

step_size = 2.0
tv_weight = 0.1
smooth_floor = 0.5
shrink_weight = 0.1

RING = 8
EARLY = 11
RING_FAR = (4, 3, 5, 2, 6, 1, 7)
CROSS_FAR = (2, 1, 3)
ALL_FAR = sorted(
    ((far, k) for far in range(4) for k in range(RING) if far or k),
    key=lambda to: -(min(to[0], 4 - to[0]) + min(to[1], RING - to[1])),
)


MESH = pl.DeviceIdType.MESH
F32 = jnp.float32
BF16 = jnp.bfloat16


def dft_tables():
    counter = np.arange(N)
    angle = (counter[:, None] * counter[None, :] % N) * (2.0 * math.pi / N)
    cosine = jnp.asarray((np.cos(angle) / math.sqrt(N)).astype(np.float32)).astype(BF16)
    sine = jnp.asarray((np.sin(angle) / math.sqrt(N)).astype(np.float32)).astype(BF16)
    return np.stack([np.asarray(cosine), np.asarray(sine), np.asarray(-sine)])


def mm(a, b):
    return jnp.dot(a, b, preferred_element_type=F32)


def mm_nt(a, b):
    return lax.dot_general(a, b, (((1,), (1,)), ((), ())), preferred_element_type=F32)


def taps_of(first, offset, taps):
    distance = lax.broadcasted_iota(jnp.int32, (N, BS), 0) - (first + offset)
    matrix = jnp.zeros((N, BS), F32)
    for tap in range(KW):
        matrix = jnp.where(distance == tap, taps[tap : tap + 1, :], matrix)
    return matrix.astype(BF16)


def swap_lanes(field):
    lane = lax.broadcasted_iota(jnp.int32, field.shape, 1)
    width = field.shape[1]
    return jnp.where(
        lane % 2 == 0, pltpu.roll(field, width - 1, 1), pltpu.roll(field, 1, 1)
    )


def swap_rows(field):
    row = lax.broadcasted_iota(jnp.int32, field.shape, 0)
    height = field.shape[0]
    return jnp.where(
        row % 2 == 0, pltpu.roll(field, height - 1, 0), pltpu.roll(field, 1, 0)
    )


def shrunk(real, imag, limit):
    length = jnp.sqrt(real * real + imag * imag)
    factor = jnp.maximum(length - limit, 0.0) / jnp.maximum(length, limit)
    return real * factor, imag * factor


def wavelet_prox(real, imag, limit):
    parts = []
    for field in (real, imag):
        across = swap_lanes(field)
        down = swap_rows(field)
        both = swap_lanes(down)
        parts.append(
            (
                (field + across + down + both) * 0.5,
                (field - across + down - both) * 0.5,
                (field + across - down - both) * 0.5,
                (field - across - down + both) * 0.5,
            )
        )
    out_real, out_imag = parts[0][0], parts[1][0]
    for band in range(1, 4):
        band_real, band_imag = shrunk(parts[0][band], parts[1][band], limit)
        out_real = out_real + band_real
        out_imag = out_imag + band_imag
    return out_real * 0.5, out_imag * 0.5


def slope(late, early):
    real = late[0] - early[0]
    imag = late[1] - early[1]
    length = jnp.sqrt(real * real + imag * imag + smooth_floor * smooth_floor)
    return real / length, imag / length


def kernel(
    coils,
    frames,
    image_hbm,
    maps_hbm,
    samples_hbm,
    used_hbm,
    row_off_hbm,
    col_off_hbm,
    row_first_hbm,
    col_first_hbm,
    row_taps_hbm,
    col_taps_hbm,
    table_hbm,
    out_ref,
    misfit_ref,
    image_ref,
    maps_ref,
    samples_ref,
    used_ref,
    row_off_ref,
    col_off_ref,
    row_first_ref,
    col_first_ref,
    row_taps_ref,
    col_taps_ref,
    table_ref,
    current,
    low,
    gathered,
    beside,
    adjoint,
    part_out,
    part_in,
    mis_out,
    mis_in,
    mis_mid,
    mis_end,
    wx,
    wy,
    kspace,
    weighted,
    back,
    local_sem,
    all_send,
    all_recv,
    side_send,
    side_recv,
    mis_send,
    mis_recv,
):
    me = lax.axis_index("coil")
    frame = lax.axis_index("frame")
    columns = coils // RING
    my_z = lax.rem(me, RING)
    my_x = me // RING
    height = N // coils

    def ring_coil(k):
        return my_x * RING + lax.rem(my_z + k, RING)

    def cross_x(k):
        return lax.rem(my_x + k, columns)

    def cross_coil(k):
        return cross_x(k) * RING + my_z

    def any_coil(far, k):
        return cross_x(far) * RING + lax.rem(my_z + k, RING)

    after = lax.rem(frame + 1, frames)
    before = lax.rem(frame + frames - 1, frames)

    fetches = []
    for slot, (source, target) in enumerate(
        (
            (image_hbm, image_ref),
            (row_off_hbm, row_off_ref),
            (row_first_hbm, row_first_ref),
            (row_taps_hbm, row_taps_ref),
            (col_off_hbm, col_off_ref),
            (col_first_hbm, col_first_ref),
            (col_taps_hbm, col_taps_ref),
            (maps_hbm, maps_ref),
            (table_hbm, table_ref),
            (samples_hbm, samples_ref),
            (used_hbm, used_ref),
        )
    ):
        fetch = pltpu.make_async_copy(source, target, local_sem.at[slot])
        fetch.start()
        fetches.append(fetch)

    barrier = pltpu.get_barrier_semaphore()
    for k in RING_FAR:
        pl.semaphore_signal(
            barrier, inc=1, device_id={"coil": ring_coil(k)}, device_id_type=MESH
        )
    for k in CROSS_FAR:
        pl.semaphore_signal(
            barrier, inc=1, device_id={"coil": cross_coil(k)}, device_id_type=MESH
        )
    for side in (after, before):
        pl.semaphore_signal(barrier, inc=1, device_id={"frame": side}, device_id_type=MESH)

    leaving = []

    def drain():
        for copy in leaving:
            copy.wait_send()
        leaving.clear()

    def send(source, target, send_sem, recv_sem, device):
        copy = pltpu.make_async_remote_copy(
            src_ref=source,
            dst_ref=target,
            send_sem=send_sem,
            recv_sem=recv_sem,
            device_id=device,
            device_id_type=MESH,
        )
        copy.start()
        leaving.append(copy)
        return copy

    fetches[0].wait()
    for part in range(2):
        current[0, part] = image_ref[:, part, :]
        low[0, part] = image_ref[:, part, :].astype(BF16)

    def build(first_ref, off_ref, taps_ref, out, b, carry):
        out[b] = taps_of(first_ref[b], off_ref[0, b], taps_ref[b].astype(F32))
        return carry

    def build_rows(start, stop):
        lax.fori_loop(
            start, stop, functools.partial(build, row_first_ref, row_off_ref, row_taps_ref, wx), 0
        )

    def build_columns(start, stop):
        lax.fori_loop(
            start, stop, functools.partial(build, col_first_ref, col_off_ref, col_taps_ref, wy), 0
        )

    for fetch in fetches[1:4]:
        fetch.wait()
    build_rows(0, EARLY)
    pl.semaphore_wait(barrier, RING - 1 + columns - 1 + 2)

    for step in range(ITERS):
        sides = [
            send(
                current.at[step],
                beside.at[step, slot],
                side_send.at[step, slot],
                side_recv.at[step, slot],
                {"frame": side},
            )
            for slot, side in ((0, after), (1, before))
        ]
        gathered[step, me] = low[step]
        if step == 0:
            cross = []
            for k in RING_FAR:
                send(
                    low.at[step],
                    gathered.at[step, me],
                    all_send.at[2 * step, 0, k],
                    all_recv.at[2 * step, 0, k],
                    {"coil": ring_coil(k)},
                )

            def arrival(k):
                return pltpu.make_async_remote_copy(
                    src_ref=low.at[step],
                    dst_ref=gathered.at[step, ring_coil(RING - k)],
                    send_sem=all_send.at[2 * step, 0, k],
                    recv_sem=all_recv.at[2 * step, 0, k],
                    device_id={"coil": ring_coil(k)},
                    device_id_type=MESH,
                )

            def forward(k, source):
                for far in CROSS_FAR:
                    copy = send(
                        source,
                        gathered.at[step, ring_coil(RING - k)],
                        all_send.at[2 * step, far, k],
                        all_recv.at[2 * step, far, k],
                        {"coil": cross_coil(far)},
                    )
                    cross.append(copy)

            forward(0, low.at[step])
            for fetch in fetches[4:7]:
                fetch.wait()
            build_rows(EARLY, NB)
            build_columns(0, NB)
            for place in range(RING - 1):
                sender = place + (my_z <= place).astype(jnp.int32)
                k = lax.rem(my_z + RING - sender, RING)
                arrival(k).wait_recv()
                forward(k, gathered.at[step, my_x * RING + sender])
            for fetch in fetches[7:]:
                fetch.wait()
            for copy in cross:
                copy.wait_recv()
        else:
            copies = [
                send(
                    low.at[step],
                    gathered.at[step, me],
                    all_send.at[2 * step, far, k],
                    all_recv.at[2 * step, far, k],
                    {"coil": any_coil(far, k)},
                )
                for far, k in ALL_FAR
            ]
            drain()
            for copy in copies:
                copy.wait_recv()

        cosine, sine, minus = table_ref[0], table_ref[1], table_ref[2]
        map_real = maps_ref[0].astype(F32)
        map_imag = maps_ref[1].astype(F32)
        image_real = gathered[step, :, 0].astype(F32).reshape(N, N)
        image_imag = gathered[step, :, 1].astype(F32).reshape(N, N)
        coil_real = (map_real * image_real - map_imag * image_imag).astype(BF16)
        coil_imag = (map_real * image_imag + map_imag * image_real).astype(BF16)
        half_real = (mm(cosine, coil_real) + mm(sine, coil_imag)).astype(BF16)
        half_imag = (mm(cosine, coil_imag) + mm(minus, coil_real)).astype(BF16)
        kspace[0:N] = (mm(half_real, cosine) + mm(half_imag, sine)).astype(BF16)
        kspace[N : 2 * N] = (mm(half_imag, cosine) + mm(half_real, minus)).astype(BF16)

        def visit(b, misfit):
            rows = wx[b]
            wide = rows.astype(F32)
            measured = samples_ref[b].astype(F32)
            active = jnp.full((1, BS), b, jnp.int32) < used_ref[0]
            for part in range(2):
                across = mm(kspace[part * N : part * N + N], wy[b])
                predicted = jnp.sum(across * wide, axis=0, keepdims=True)
                resid = jnp.where(active, predicted - measured[part : part + 1], 0.0)
                misfit = misfit + resid * resid
                weighted[b, part * N : part * N + N] = resid.astype(BF16) * rows
            return misfit

        misfit = jnp.zeros((1, BS), F32)
        for b in range(NB):
            misfit = visit(b, misfit)
        mis_out[step : step + 1, :] = misfit

        if step == ITERS - 1:
            mis_cross = [
                send(
                    mis_out,
                    mis_in.at[far],
                    mis_send.at[0, far],
                    mis_recv.at[0, far],
                    {"coil": cross_coil(far)},
                )
                for far in CROSS_FAR
            ]

        totals = []
        for part in range(2):
            total = mm_nt(weighted[0, part * N : part * N + N], wy[0])
            for b in range(1, NB):
                total = total + mm_nt(weighted[b, part * N : part * N + N], wy[b])
            totals.append(total.astype(BF16))
        grid_real, grid_imag = totals
        back[0] = (mm(cosine, grid_real) + mm(minus, grid_imag)).astype(BF16)
        back[1] = (mm(cosine, grid_imag) + mm(sine, grid_real)).astype(BF16)
        copies = []
        for pair in ((2, 1), (3, 0)):
            strips = [
                pl.ds(pl.multiple_of(cross_x(far) * RING * height, RING * height), RING * height)
                for far in pair
            ]

            def taken(ref, part):
                return jnp.concatenate([ref[part, strip] for strip in strips], axis=0)

            back_real, back_imag = taken(back, 0), taken(back, 1)
            map_real = taken(maps_ref, 0).astype(F32)
            map_imag = taken(maps_ref, 1).astype(F32)
            coil_real = mm(back_real, cosine) + mm(back_imag, minus)
            coil_imag = mm(back_imag, cosine) + mm(back_real, sine)
            for part, field in enumerate(
                (
                    map_real * coil_real + map_imag * coil_imag,
                    map_real * coil_imag - map_imag * coil_real,
                )
            ):
                shards = field.reshape(2, RING, height, N)
                for place, far in enumerate(pair):
                    part_out[step, far, :, part] = shards[place].astype(BF16)
                    if far == 0:
                        adjoint[:, part] = shards[place]
            for far in pair:
                for k in RING_FAR + (0,):
                    if far or k:
                        copies.append(
                            send(
                                part_out.at[step, far, lax.rem(my_z + k, RING)],
                                part_in.at[step, far, k],
                                all_send.at[2 * step + 1, far, k],
                                all_recv.at[2 * step + 1, far, k],
                                {"coil": any_coil(far, k)},
                            )
                        )

        if step == ITERS - 1:
            for copy in mis_cross:
                copy.wait_recv()
            mis_sum = mis_out[...]
            for far in CROSS_FAR:
                mis_sum = mis_sum + mis_in[far]
            mis_mid[...] = mis_sum
            mis_ring = [
                send(
                    mis_mid,
                    mis_end.at[k],
                    mis_send.at[1, k],
                    mis_recv.at[1, k],
                    {"coil": ring_coil(k)},
                )
                for k in RING_FAR
            ]
        for copy in sides:
            copy.wait_recv()
        here = (current[step, 0], current[step, 1])
        early = (beside[step, 0, 0], beside[step, 0, 1])
        late = (beside[step, 1, 0], beside[step, 1, 1])
        first = slope(here, early)
        second = slope(late, here)
        pieces = adjoint[my_z]
        for copy in copies:
            copy.wait_recv()
        for far in range(columns):
            for k in range(RING):
                if far or k:
                    pieces = pieces + part_in[step, far, k].astype(F32)
        result = [
            here[part]
            - step_size * (pieces[part] + tv_weight * (first[part] - second[part]))
            for part in range(2)
        ]
        result = wavelet_prox(result[0], result[1], step_size * shrink_weight)
        for part in range(2):
            if step < ITERS - 1:
                current[step + 1, part] = result[part]
                low[step + 1, part] = result[part].astype(BF16)
            else:
                out_ref[:, part, :] = result[part]

    for copy in mis_ring:
        copy.wait_recv()
    for k in RING_FAR:
        mis_sum = mis_sum + mis_end[k]
    mis_sum = jnp.sum(mis_sum, axis=1, keepdims=True) * (0.5 / (coils * NB * BS))
    lane = lax.broadcasted_iota(jnp.int32, (1, ITERS), 1)
    misfit_ref[...] = jnp.where(lane == 0, mis_sum[0:1], mis_sum[1:2])
    drain()


def solution(mesh):
    coils = mesh.shape["coil"]
    frames = mesh.shape["frame"]
    columns = coils // RING
    height = N // coils
    tables = dft_tables()
    vmem = pl.BlockSpec(memory_space=pltpu.VMEM)
    hbm = pl.BlockSpec(memory_space=pltpu.HBM)

    def on_device(
        initial_image,
        coil_maps,
        samples,
        blocks_used,
        row_offset,
        col_offset,
        row_first,
        col_first,
        row_taps,
        col_taps,
    ):
        image, misfit = pl.pallas_call(
            functools.partial(kernel, coils, frames),
            out_shape=(
                pltpu.VMEM((height, 2, N), F32),
                pltpu.VMEM((1, ITERS), F32),
            ),
            in_specs=[hbm] * 11,
            out_specs=(vmem, vmem),
            scratch_shapes=[
                pltpu.VMEM((height, 2, N), F32),
                pltpu.VMEM((2, N, N), BF16),
                pltpu.VMEM((NB, 2, BS), BF16),
                pltpu.SMEM((1,), jnp.int32),
                pltpu.SMEM((1, NB), jnp.int32),
                pltpu.SMEM((1, NB), jnp.int32),
                pltpu.VMEM((NB, 1, BS), jnp.int32),
                pltpu.VMEM((NB, 1, BS), jnp.int32),
                pltpu.VMEM((NB, KW, BS), BF16),
                pltpu.VMEM((NB, KW, BS), BF16),
                pltpu.VMEM((3, N, N), BF16),
                pltpu.VMEM((ITERS, 2, height, N), F32),
                pltpu.VMEM((ITERS, 2, height, N), BF16),
                pltpu.VMEM((ITERS, coils, 2, height, N), BF16),
                pltpu.VMEM((ITERS, 2, 2, height, N), F32),
                pltpu.VMEM((RING, 2, height, N), F32),
                pltpu.VMEM((ITERS, columns, RING, 2, height, N), BF16),
                pltpu.VMEM((ITERS, columns, RING, 2, height, N), BF16),
                pltpu.VMEM((ITERS, BS), F32),
                pltpu.VMEM((columns, ITERS, BS), F32),
                pltpu.VMEM((ITERS, BS), F32),
                pltpu.VMEM((RING, ITERS, BS), F32),
                pltpu.VMEM((NB, N, BS), BF16),
                pltpu.VMEM((NB, N, BS), BF16),
                pltpu.VMEM((2 * N, N), BF16),
                pltpu.VMEM((NB, 2 * N, BS), BF16),
                pltpu.VMEM((2, N, N), BF16),
                pltpu.SemaphoreType.DMA((11,)),
                pltpu.SemaphoreType.DMA((2 * ITERS, columns, RING)),
                pltpu.SemaphoreType.DMA((2 * ITERS, columns, RING)),
                pltpu.SemaphoreType.DMA((ITERS, 2)),
                pltpu.SemaphoreType.DMA((ITERS, 2)),
                pltpu.SemaphoreType.DMA((2, RING)),
                pltpu.SemaphoreType.DMA((2, RING)),
            ],
            compiler_params=pltpu.CompilerParams(
                collective_id=0, has_side_effects=True, vmem_limit_bytes=67043328 - 32 * 1024
            ),
        )(
            initial_image[:, 0],
            coil_maps[0],
            samples[0, 0],
            blocks_used,
            row_offset,
            col_offset,
            row_first[0][:, None],
            col_first[0][:, None],
            row_taps[0],
            col_taps[0],
            tables,
        )
        return image[:, None], misfit.T

    placed = (
        P("coil", "frame", None, None),
        P("coil", None, None, None),
        P("coil", "frame", None, None, None),
        P("frame"),
        P("frame", None),
        P("frame", None),
        P("frame", None, None),
        P("frame", None, None),
        P("frame", None, None, None),
        P("frame", None, None, None),
    )
    return jax.shard_map(
        on_device,
        mesh=mesh,
        in_specs=placed,
        out_specs=(P("coil", "frame", None, None), P(None, "frame")),
        check_vma=False,
    )
```

```python
import functools
import math

import jax
import jax.numpy as jnp
import numpy as np
from jax import lax
from jax.experimental import pallas as pl
from jax.experimental.pallas import tpu as pltpu
from jax.sharding import PartitionSpec as P

N = 256
NB = 18
BS = 256
KW = 4
ITERS = 2

step_size = 2.0
tv_weight = 0.1
smooth_floor = 0.5
shrink_weight = 0.1

RING = 8
EARLY = 11
RING_FAR = (4, 3, 5, 2, 6, 1, 7)
CROSS_FAR = (2, 1, 3)
ALL_FAR = sorted(
    ((far, k) for far in range(4) for k in range(RING) if far or k),
    key=lambda to: -(min(to[0], 4 - to[0]) + min(to[1], RING - to[1])),
)


MESH = pl.DeviceIdType.MESH
F32 = jnp.float32
BF16 = jnp.bfloat16


def dft_tables():
    counter = np.arange(N)
    angle = (counter[:, None] * counter[None, :] % N) * (2.0 * math.pi / N)
    cosine = jnp.asarray((np.cos(angle) / math.sqrt(N)).astype(np.float32)).astype(BF16)
    sine = jnp.asarray((np.sin(angle) / math.sqrt(N)).astype(np.float32)).astype(BF16)
    return np.stack([np.asarray(cosine), np.asarray(sine), np.asarray(-sine)])


def mm(a, b):
    return jnp.dot(a, b, preferred_element_type=F32)


def mm_nt(a, b):
    return lax.dot_general(a, b, (((1,), (1,)), ((), ())), preferred_element_type=F32)


def taps_of(first, offset, taps):
    distance = lax.broadcasted_iota(jnp.int32, (N, BS), 0) - (first + offset)
    matrix = jnp.zeros((N, BS), F32)
    for tap in range(KW):
        matrix = jnp.where(distance == tap, taps[tap : tap + 1, :], matrix)
    return matrix.astype(BF16)


def swap_lanes(field):
    lane = lax.broadcasted_iota(jnp.int32, field.shape, 1)
    width = field.shape[1]
    return jnp.where(
        lane % 2 == 0, pltpu.roll(field, width - 1, 1), pltpu.roll(field, 1, 1)
    )


def swap_rows(field):
    row = lax.broadcasted_iota(jnp.int32, field.shape, 0)
    height = field.shape[0]
    return jnp.where(
        row % 2 == 0, pltpu.roll(field, height - 1, 0), pltpu.roll(field, 1, 0)
    )


def shrunk(real, imag, limit):
    length = jnp.sqrt(real * real + imag * imag)
    factor = jnp.maximum(length - limit, 0.0) / jnp.maximum(length, limit)
    return real * factor, imag * factor


def wavelet_prox(real, imag, limit):
    parts = []
    for field in (real, imag):
        across = swap_lanes(field)
        down = swap_rows(field)
        both = swap_lanes(down)
        parts.append(
            (
                (field + across + down + both) * 0.5,
                (field - across + down - both) * 0.5,
                (field + across - down - both) * 0.5,
                (field - across - down + both) * 0.5,
            )
        )
    out_real, out_imag = parts[0][0], parts[1][0]
    for band in range(1, 4):
        band_real, band_imag = shrunk(parts[0][band], parts[1][band], limit)
        out_real = out_real + band_real
        out_imag = out_imag + band_imag
    return out_real * 0.5, out_imag * 0.5


def slope(late, early):
    real = late[0] - early[0]
    imag = late[1] - early[1]
    length = jnp.sqrt(real * real + imag * imag + smooth_floor * smooth_floor)
    return real / length, imag / length


def kernel(
    coils,
    frames,
    image_hbm,
    maps_hbm,
    samples_hbm,
    used_hbm,
    row_off_hbm,
    col_off_hbm,
    row_first_hbm,
    col_first_hbm,
    row_taps_hbm,
    col_taps_hbm,
    table_hbm,
    out_ref,
    misfit_ref,
    image_ref,
    maps_ref,
    samples_ref,
    used_ref,
    row_off_ref,
    col_off_ref,
    row_first_ref,
    col_first_ref,
    row_taps_ref,
    col_taps_ref,
    table_ref,
    current,
    low,
    gathered,
    beside,
    adjoint,
    part_out,
    part_in,
    mis_out,
    mis_in,
    mis_mid,
    mis_end,
    wx,
    wy,
    kspace,
    weighted,
    back,
    local_sem,
    all_send,
    all_recv,
    side_send,
    side_recv,
    mis_send,
    mis_recv,
):
    me = lax.axis_index("coil")
    frame = lax.axis_index("frame")
    columns = coils // RING
    my_z = lax.rem(me, RING)
    my_x = me // RING
    height = N // coils

    def ring_coil(k):
        return my_x * RING + lax.rem(my_z + k, RING)

    def cross_x(k):
        return lax.rem(my_x + k, columns)

    def cross_coil(k):
        return cross_x(k) * RING + my_z

    def any_coil(far, k):
        return cross_x(far) * RING + lax.rem(my_z + k, RING)

    after = lax.rem(frame + 1, frames)
    before = lax.rem(frame + frames - 1, frames)

    fetches = []
    for slot, (source, target) in enumerate(
        (
            (image_hbm, image_ref),
            (row_off_hbm, row_off_ref),
            (row_first_hbm, row_first_ref),
            (row_taps_hbm, row_taps_ref),
            (col_off_hbm, col_off_ref),
            (col_first_hbm, col_first_ref),
            (col_taps_hbm, col_taps_ref),
            (maps_hbm, maps_ref),
            (table_hbm, table_ref),
            (samples_hbm, samples_ref),
            (used_hbm, used_ref),
        )
    ):
        fetch = pltpu.make_async_copy(source, target, local_sem.at[slot])
        fetch.start()
        fetches.append(fetch)

    barrier = pltpu.get_barrier_semaphore()
    for k in RING_FAR:
        pl.semaphore_signal(
            barrier, inc=1, device_id={"coil": ring_coil(k)}, device_id_type=MESH
        )
    for k in CROSS_FAR:
        pl.semaphore_signal(
            barrier, inc=1, device_id={"coil": cross_coil(k)}, device_id_type=MESH
        )
    for side in (after, before):
        pl.semaphore_signal(barrier, inc=1, device_id={"frame": side}, device_id_type=MESH)

    leaving = []

    def drain():
        for copy in leaving:
            copy.wait_send()
        leaving.clear()

    def send(source, target, send_sem, recv_sem, device):
        copy = pltpu.make_async_remote_copy(
            src_ref=source,
            dst_ref=target,
            send_sem=send_sem,
            recv_sem=recv_sem,
            device_id=device,
            device_id_type=MESH,
        )
        copy.start()
        leaving.append(copy)
        return copy

    fetches[0].wait()
    for part in range(2):
        current[0, part] = image_ref[:, part, :]
        low[0, part] = image_ref[:, part, :].astype(BF16)

    def build(first_ref, off_ref, taps_ref, out, b, carry):
        out[b] = taps_of(first_ref[b], off_ref[0, b], taps_ref[b].astype(F32))
        return carry

    def build_rows(start, stop):
        lax.fori_loop(
            start, stop, functools.partial(build, row_first_ref, row_off_ref, row_taps_ref, wx), 0
        )

    def build_columns(start, stop):
        lax.fori_loop(
            start, stop, functools.partial(build, col_first_ref, col_off_ref, col_taps_ref, wy), 0
        )

    for fetch in fetches[1:4]:
        fetch.wait()
    build_rows(0, EARLY)
    pl.semaphore_wait(barrier, RING - 1 + columns - 1 + 2)

    for step in range(ITERS):
        sides = [
            send(
                current.at[step],
                beside.at[step, slot],
                side_send.at[step, slot],
                side_recv.at[step, slot],
                {"frame": side},
            )
            for slot, side in ((0, after), (1, before))
        ]
        gathered[step, me] = low[step]
        if step == 0:
            cross = []
            for k in RING_FAR:
                send(
                    low.at[step],
                    gathered.at[step, me],
                    all_send.at[2 * step, 0, k],
                    all_recv.at[2 * step, 0, k],
                    {"coil": ring_coil(k)},
                )

            def arrival(k):
                return pltpu.make_async_remote_copy(
                    src_ref=low.at[step],
                    dst_ref=gathered.at[step, ring_coil(RING - k)],
                    send_sem=all_send.at[2 * step, 0, k],
                    recv_sem=all_recv.at[2 * step, 0, k],
                    device_id={"coil": ring_coil(k)},
                    device_id_type=MESH,
                )

            def forward(k, source):
                for far in CROSS_FAR:
                    copy = send(
                        source,
                        gathered.at[step, ring_coil(RING - k)],
                        all_send.at[2 * step, far, k],
                        all_recv.at[2 * step, far, k],
                        {"coil": cross_coil(far)},
                    )
                    cross.append(copy)

            forward(0, low.at[step])
            for fetch in fetches[4:7]:
                fetch.wait()
            build_rows(EARLY, NB)
            build_columns(0, NB // 3)
            for place in range(RING - 1):
                sender = place + (my_z <= place).astype(jnp.int32)
                k = lax.rem(my_z + RING - sender, RING)
                arrival(k).wait_recv()
                forward(k, gathered.at[step, my_x * RING + sender])
            build_columns(NB // 3, NB)
            for fetch in fetches[7:]:
                fetch.wait()
            for copy in cross:
                copy.wait_recv()
        else:
            copies = [
                send(
                    low.at[step],
                    gathered.at[step, me],
                    all_send.at[2 * step, far, k],
                    all_recv.at[2 * step, far, k],
                    {"coil": any_coil(far, k)},
                )
                for far, k in ALL_FAR
            ]
            drain()
            for copy in copies:
                copy.wait_recv()

        cosine, sine, minus = table_ref[0], table_ref[1], table_ref[2]
        map_real = maps_ref[0].astype(F32)
        map_imag = maps_ref[1].astype(F32)
        image_real = gathered[step, :, 0].astype(F32).reshape(N, N)
        image_imag = gathered[step, :, 1].astype(F32).reshape(N, N)
        coil_real = (map_real * image_real - map_imag * image_imag).astype(BF16)
        coil_imag = (map_real * image_imag + map_imag * image_real).astype(BF16)
        half_real = (mm(cosine, coil_real) + mm(sine, coil_imag)).astype(BF16)
        half_imag = (mm(cosine, coil_imag) + mm(minus, coil_real)).astype(BF16)
        kspace[0:N] = (mm(half_real, cosine) + mm(half_imag, sine)).astype(BF16)
        kspace[N : 2 * N] = (mm(half_imag, cosine) + mm(half_real, minus)).astype(BF16)

        def visit(b, misfit):
            rows = wx[b]
            wide = rows.astype(F32)
            measured = samples_ref[b].astype(F32)
            active = jnp.full((1, BS), b, jnp.int32) < used_ref[0]
            for part in range(2):
                across = mm(kspace[part * N : part * N + N], wy[b])
                predicted = jnp.sum(across * wide, axis=0, keepdims=True)
                resid = jnp.where(active, predicted - measured[part : part + 1], 0.0)
                misfit = misfit + resid * resid
                weighted[b, part * N : part * N + N] = resid.astype(BF16) * rows
            return misfit

        misfit = jnp.zeros((1, BS), F32)
        for b in range(NB):
            misfit = visit(b, misfit)
        mis_out[step : step + 1, :] = misfit

        if step == ITERS - 1:
            mis_cross = [
                send(
                    mis_out,
                    mis_in.at[far],
                    mis_send.at[0, far],
                    mis_recv.at[0, far],
                    {"coil": cross_coil(far)},
                )
                for far in CROSS_FAR
            ]

        totals = []
        for part in range(2):
            total = mm_nt(weighted[0, part * N : part * N + N], wy[0])
            for b in range(1, NB):
                total = total + mm_nt(weighted[b, part * N : part * N + N], wy[b])
            totals.append(total.astype(BF16))
        grid_real, grid_imag = totals
        back[0] = (mm(cosine, grid_real) + mm(minus, grid_imag)).astype(BF16)
        back[1] = (mm(cosine, grid_imag) + mm(sine, grid_real)).astype(BF16)
        copies = []
        for pair in ((2, 1), (3, 0)):
            strips = [
                pl.ds(pl.multiple_of(cross_x(far) * RING * height, RING * height), RING * height)
                for far in pair
            ]

            def taken(ref, part):
                return jnp.concatenate([ref[part, strip] for strip in strips], axis=0)

            back_real, back_imag = taken(back, 0), taken(back, 1)
            map_real = taken(maps_ref, 0).astype(F32)
            map_imag = taken(maps_ref, 1).astype(F32)
            coil_real = mm(back_real, cosine) + mm(back_imag, minus)
            coil_imag = mm(back_imag, cosine) + mm(back_real, sine)
            for part, field in enumerate(
                (
                    map_real * coil_real + map_imag * coil_imag,
                    map_real * coil_imag - map_imag * coil_real,
                )
            ):
                shards = field.reshape(2, RING, height, N)
                for place, far in enumerate(pair):
                    part_out[step, far, :, part] = shards[place].astype(BF16)
                    if far == 0:
                        adjoint[:, part] = shards[place]
            for far in pair:
                for k in RING_FAR + (0,):
                    if far or k:
                        copies.append(
                            send(
                                part_out.at[step, far, lax.rem(my_z + k, RING)],
                                part_in.at[step, far, k],
                                all_send.at[2 * step + 1, far, k],
                                all_recv.at[2 * step + 1, far, k],
                                {"coil": any_coil(far, k)},
                            )
                        )

        if step == ITERS - 1:
            for copy in mis_cross:
                copy.wait_recv()
            mis_sum = mis_out[...]
            for far in CROSS_FAR:
                mis_sum = mis_sum + mis_in[far]
            mis_mid[...] = mis_sum
            mis_ring = [
                send(
                    mis_mid,
                    mis_end.at[k],
                    mis_send.at[1, k],
                    mis_recv.at[1, k],
                    {"coil": ring_coil(k)},
                )
                for k in RING_FAR
            ]
        for copy in sides:
            copy.wait_recv()
        here = (current[step, 0], current[step, 1])
        early = (beside[step, 0, 0], beside[step, 0, 1])
        late = (beside[step, 1, 0], beside[step, 1, 1])
        first = slope(here, early)
        second = slope(late, here)
        pieces = adjoint[my_z]
        for copy in copies:
            copy.wait_recv()
        for far in range(columns):
            for k in range(RING):
                if far or k:
                    pieces = pieces + part_in[step, far, k].astype(F32)
        result = [
            here[part]
            - step_size * (pieces[part] + tv_weight * (first[part] - second[part]))
            for part in range(2)
        ]
        result = wavelet_prox(result[0], result[1], step_size * shrink_weight)
        for part in range(2):
            if step < ITERS - 1:
                current[step + 1, part] = result[part]
                low[step + 1, part] = result[part].astype(BF16)
            else:
                out_ref[:, part, :] = result[part]

    for copy in mis_ring:
        copy.wait_recv()
    for k in RING_FAR:
        mis_sum = mis_sum + mis_end[k]
    mis_sum = jnp.sum(mis_sum, axis=1, keepdims=True) * (0.5 / (coils * NB * BS))
    lane = lax.broadcasted_iota(jnp.int32, (1, ITERS), 1)
    misfit_ref[...] = jnp.where(lane == 0, mis_sum[0:1], mis_sum[1:2])
    drain()


def solution(mesh):
    coils = mesh.shape["coil"]
    frames = mesh.shape["frame"]
    columns = coils // RING
    height = N // coils
    tables = dft_tables()
    vmem = pl.BlockSpec(memory_space=pltpu.VMEM)
    hbm = pl.BlockSpec(memory_space=pltpu.HBM)

    def on_device(
        initial_image,
        coil_maps,
        samples,
        blocks_used,
        row_offset,
        col_offset,
        row_first,
        col_first,
        row_taps,
        col_taps,
    ):
        image, misfit = pl.pallas_call(
            functools.partial(kernel, coils, frames),
            out_shape=(
                pltpu.VMEM((height, 2, N), F32),
                pltpu.VMEM((1, ITERS), F32),
            ),
            in_specs=[hbm] * 11,
            out_specs=(vmem, vmem),
            scratch_shapes=[
                pltpu.VMEM((height, 2, N), F32),
                pltpu.VMEM((2, N, N), BF16),
                pltpu.VMEM((NB, 2, BS), BF16),
                pltpu.SMEM((1,), jnp.int32),
                pltpu.SMEM((1, NB), jnp.int32),
                pltpu.SMEM((1, NB), jnp.int32),
                pltpu.VMEM((NB, 1, BS), jnp.int32),
                pltpu.VMEM((NB, 1, BS), jnp.int32),
                pltpu.VMEM((NB, KW, BS), BF16),
                pltpu.VMEM((NB, KW, BS), BF16),
                pltpu.VMEM((3, N, N), BF16),
                pltpu.VMEM((ITERS, 2, height, N), F32),
                pltpu.VMEM((ITERS, 2, height, N), BF16),
                pltpu.VMEM((ITERS, coils, 2, height, N), BF16),
                pltpu.VMEM((ITERS, 2, 2, height, N), F32),
                pltpu.VMEM((RING, 2, height, N), F32),
                pltpu.VMEM((ITERS, columns, RING, 2, height, N), BF16),
                pltpu.VMEM((ITERS, columns, RING, 2, height, N), BF16),
                pltpu.VMEM((ITERS, BS), F32),
                pltpu.VMEM((columns, ITERS, BS), F32),
                pltpu.VMEM((ITERS, BS), F32),
                pltpu.VMEM((RING, ITERS, BS), F32),
                pltpu.VMEM((NB, N, BS), BF16),
                pltpu.VMEM((NB, N, BS), BF16),
                pltpu.VMEM((2 * N, N), BF16),
                pltpu.VMEM((NB, 2 * N, BS), BF16),
                pltpu.VMEM((2, N, N), BF16),
                pltpu.SemaphoreType.DMA((11,)),
                pltpu.SemaphoreType.DMA((2 * ITERS, columns, RING)),
                pltpu.SemaphoreType.DMA((2 * ITERS, columns, RING)),
                pltpu.SemaphoreType.DMA((ITERS, 2)),
                pltpu.SemaphoreType.DMA((ITERS, 2)),
                pltpu.SemaphoreType.DMA((2, RING)),
                pltpu.SemaphoreType.DMA((2, RING)),
            ],
            compiler_params=pltpu.CompilerParams(
                collective_id=0, has_side_effects=True, vmem_limit_bytes=67043328 - 32 * 1024
            ),
        )(
            initial_image[:, 0],
            coil_maps[0],
            samples[0, 0],
            blocks_used,
            row_offset,
            col_offset,
            row_first[0][:, None],
            col_first[0][:, None],
            row_taps[0],
            col_taps[0],
            tables,
        )
        return image[:, None], misfit.T

    placed = (
        P("coil", "frame", None, None),
        P("coil", None, None, None),
        P("coil", "frame", None, None, None),
        P("frame"),
        P("frame", None),
        P("frame", None),
        P("frame", None, None),
        P("frame", None, None),
        P("frame", None, None, None),
        P("frame", None, None, None),
    )
    return jax.shard_map(
        on_device,
        mesh=mesh,
        in_specs=placed,
        out_specs=(P("coil", "frame", None, None), P(None, "frame")),
        check_vma=False,
    )
```
